256 devices in a mesh: ta: 16 (over x_lo, y, core), xyz: 16 (over x_hi, z).
Axes of the slice: x: 4 (x_hi: 2, x_lo: 2; x = x_hi * 2 + x_lo), y: 4, z: 8, core: 2. Of those that a mesh axis runs over, the one named last changes fastest.
Arguments:
- prop_one: bfloat16 [16, 2, 12, 12, 32768], P('ta', None, None, None, 'xyz'), may hold values from -1.796875 to 1.796875
- prop_two: bfloat16 [16, 2, 12, 12, 32768], P('ta', None, None, None, 'xyz'), may hold values from -1.796875 to 1.796875
Outputs:
- momentum_fields: float32 [16, 16, 2, 32768], P(None, 'ta', None, 'xyz')
The draws below stay inside these ranges and needn't reach their ends.
All inputs are finite; a program needn't handle non-finite values.
Results may differ from the reference program's by a relative error of at most 0.0003.
Values sent between devices are 32-bit elements; how exact they have to be, the bound alone decides.
A program may use at most 128 MiB of HBM per device.

```python
import jax
import jax.numpy as jnp
import numpy as np
from jax import lax

L = 32
TIMES = 16
SITES = 32768


def level_of(key, extent, split, low, top_value):
    loudness, own = 1.0, jax.random.fold_in(key, 6)
    for axis_at, parts in split:
        heights = jnp.exp(jax.random.uniform(jax.random.fold_in(own, axis_at), (parts,), jnp.float32, low / len(split), top_value / len(split)))
        loudness = loudness * jnp.repeat(heights, extent[axis_at] // parts).reshape([-1 if axis == axis_at else 1 for axis in range(len(extent))])
    return loudness


def centred(own_key, shape, spread, limit, cuts=(), dtype=jnp.bfloat16):
    factor_of = level_of(own_key, shape, cuts, -0.22, 0.18) if cuts else 1.0
    values = jax.random.normal(own_key, shape, jnp.float32) * spread * factor_of
    return jnp.minimum(jnp.maximum(values, -limit), limit).astype(dtype)


def setup_inputs(seed: int = 0) -> dict:
    seeds = jax.random.split(jax.random.key(seed), 3)
    return {
        "prop_one": centred(seeds[0], (TIMES, 2, 12, 12, SITES), 0.2887, 1.796875, ((0, 16), (4, 16))),
        "prop_two": centred(seeds[1], (TIMES, 2, 12, 12, SITES), 0.2887, 1.796875, ((0, 16), (4, 16))),
    }


spin_columns = [[3, 2, 1, 0], [3, 2, 1, 0], [2, 3, 0, 1], [2, 3, 0, 1]]
spin_phases = [[1j, 1j, -1j, -1j], [-1.0, 1.0, 1.0, -1.0], [1j, -1j, -1j, 1j], [1.0, 1.0, 1.0, 1.0]]
chiral_signs = [1.0, 1.0, -1.0, -1.0]


def vertex_parts():
    result = []
    for gamma_index in range(4):
        columns = spin_columns[gamma_index]
        phases = spin_phases[gamma_index]
        rows_list = [columns[a // 3] * 3 + a % 3 for a in range(12)]
        phase_list = [complex(phases[a // 3]) for a in range(12)]
        result.append((rows_list, phase_list))
    return result, [chiral_signs[a // 3] for a in range(12)]


def build_operands(prop_a, prop_b):
    gammas, chirality = vertex_parts()
    left_real, left_imag, right_real, right_imag = [], [], [], []
    for rows_list, phase_list in gammas:
        pick_real = jnp.stack([prop_a[0, q] for q in rows_list])
        pick_imag = jnp.stack([prop_a[1, q] for q in rows_list])
        phase_real = jnp.asarray(np.array([p.real for p in phase_list]), jnp.bfloat16)[:, None, None]
        phase_imag = jnp.asarray(np.array([p.imag for p in phase_list]), jnp.bfloat16)[:, None, None]
        left_real.append(phase_real * pick_real - phase_imag * pick_imag)
        left_imag.append(phase_real * pick_imag + phase_imag * pick_real)
        col_real = jnp.stack([prop_b[0][:, q] for q in rows_list], axis=1)
        col_imag = jnp.stack([prop_b[1][:, q] for q in rows_list], axis=1)
        factor = np.array([[phase_list[c] * chirality[rows_list[c]] * chirality[a] for c in range(12)] for a in range(12)])
        factor_real = jnp.asarray(factor.real, jnp.bfloat16)[:, :, None]
        factor_imag = jnp.asarray(factor.imag, jnp.bfloat16)[:, :, None]
        right_real.append(factor_real * col_real + factor_imag * col_imag)
        right_imag.append(factor_imag * col_real - factor_real * col_imag)
    left_rows = jnp.stack(left_real + left_imag).reshape(8, 144, -1)
    right_rows = jnp.stack(right_real + right_imag).reshape(8, 144, -1)
    return left_rows, right_rows


def combine_products(products):
    real_sum = products[:4, :4] - products[4:, 4:]
    imag_sum = products[:4, 4:] + products[4:, :4]
    return jnp.stack([real_sum.reshape(16, -1), imag_sum.reshape(16, -1)], axis=1)


def contract(prop_a, prop_b):
    left_rows, right_rows = build_operands(prop_a, prop_b)
    products = jnp.einsum("mks,nks->mns", left_rows.astype(jnp.float32), right_rows.astype(jnp.float32))
    return combine_products(products)


def reference(prop_one, prop_two):
    def per_slice(slice_pair):
        first_planes = jnp.moveaxis(slice_pair[0].reshape(2, 12, 12, L, L * L), 3, 0)
        second_planes = jnp.moveaxis(slice_pair[1].reshape(2, 12, 12, L, L * L), 3, 0)
        fields = lax.map(lambda plane_pair: contract(plane_pair[0], plane_pair[1]), (first_planes, second_planes))
        fields = jnp.moveaxis(fields, 0, 2).reshape(16, 2, L * L * L)
        complex_field = lax.complex(fields[:, 0], fields[:, 1]).reshape(16, L, L, L)
        spectrum = jnp.fft.fftn(complex_field, axes=(1, 2, 3), norm="ortho")
        spectrum = jnp.transpose(spectrum, (0, 2, 3, 1)).reshape(16, L * L * L)
        return jnp.stack([jnp.real(spectrum), jnp.imag(spectrum)], axis=1).astype(jnp.float32)

    return lax.map(per_slice, (prop_one, prop_two))
```

```python
import functools

import jax
import jax.numpy as jnp
import numpy as np
from jax import lax
from jax.experimental import pallas as pl
from jax.experimental.pallas import tpu as pltpu
from jax.sharding import PartitionSpec as P

L = 32
MESH = pl.DeviceIdType.MESH
ENTRIES = 144
PITCH = 32

REVERSED = [3, 2, 1, 0]
SWAPPED = [2, 3, 0, 1]
LEFT_PHASE = [1j, -1.0, 1j, 1.0]
RIGHT_PHASE = [-1j, 1.0, -1j, -1.0]


def split_table(values):
    high = jnp.asarray(values, jnp.float32).astype(jnp.bfloat16)
    high_np = np.asarray(values, np.float32).astype(jnp.bfloat16).astype(np.float64)
    low = np.asarray(values - high_np, np.float32).astype(jnp.bfloat16)
    high = np.asarray(values, np.float32).astype(jnp.bfloat16)
    return high, low


def real_form(z):
    return np.stack([np.stack([z.real, -z.imag]), np.stack([z.imag, z.real])])


def fold_tables():
    result = []
    for chunk in range(2):
        table = np.zeros((2, 2, 4, 2, 8, 2, 8, 2, 8))
        for f8 in range(8):
            mu, nu = f8 // 2, 2 * chunk + f8 % 2
            phase = LEFT_PHASE[mu] * RIGHT_PHASE[nu]
            for parity in range(2):
                for m in range(4):
                    z = phase * np.exp(-2j * np.pi * np.arange(8) * (2 * m + parity) / 8)
                    form = real_form(z)
                    for x in range(2):
                        table[parity, :, m, x, f8, x, f8] = form
        result.append(np.concatenate(split_table(table.reshape(256, 256)), axis=0))
    return np.stack(result)


def twiddle_tables():
    kl = (2 * np.arange(4)[None, :] + np.arange(2)[:, None]).reshape(8)
    angle = 2 * np.pi * kl[:, None] * np.repeat(np.arange(4), 32)[None, :] / 32
    rows = np.stack([np.cos(angle), np.sin(angle)])
    return np.repeat(rows[:, :, None, :], 8, axis=2).reshape(2, 64, 128).astype(np.float32)


def plane_tables():
    yl, z = np.arange(4)[:, None], np.arange(32)[None, :]
    kz = np.array([4 * high + low for low in range(4) for high in range(8)])
    result = []
    for parity in range(2):
        table = np.zeros((2, 128, 2, 4, 32))
        for tile in range(2):
            for slot in range(4):
                part, kh = slot // 2, 2 * tile + (slot % 2 if parity == 0 else 1 - slot % 2)
                w = np.exp(-2j * np.pi * ((yl * kh / 4)[:, :, None] + z[:, :, None] * kz[None, None, :] / 32)) / 32
                form = real_form(w.reshape(128, 32))
                table[:, :, tile, slot] = form[part]
        result.append(np.stack(split_table(table.reshape(256, 256))))
    return np.stack(result)


def line_tables():
    w = np.exp(-2j * np.pi * np.arange(32)[:, None] * np.arange(32)[None, :] / 32) / np.sqrt(32)
    form = real_form(w)
    table = np.zeros((2, 4, 32, 2, 4, 32))
    for f4 in range(4):
        table[:, f4, :, :, f4] = form.transpose(1, 2, 0, 3)
    return np.stack(split_table(table.reshape(256, 256)))


def split_values(values):
    high = values.astype(jnp.bfloat16)
    low = (values - high.astype(jnp.float32)).astype(jnp.bfloat16)
    return high, low


def dot(a, b):
    return jnp.dot(a, b, preferred_element_type=jnp.float32)


def wide_dot(values, high_table, low_table):
    rows = values.shape[0]
    high, low = split_values(values)
    both = dot(jnp.concatenate([high, low], axis=0), high_table)
    return both[:rows] + both[rows:] + dot(high, low_table)


def widen(chunk, staged, sites):
    rows = 36 * PITCH
    base = chunk * rows

    def one(index, carry):
        start = pl.multiple_of(base + index * 128, 128)
        sites[pl.ds(start, 128), :] = staged[pl.ds(start, 128), :].astype(jnp.float32)
        return carry

    lax.fori_loop(0, rows // 128, one, 0)


def contract_half(chunk, sites, fields):
    right_pair = [REVERSED, SWAPPED][chunk]

    def one_plane(h, carry):
        def entry(prop, part, row, column):
            start = (prop * ENTRIES + row * 12 + column) * PITCH + part
            return sites[pl.ds(start + 16 * h, 8, stride=2), :]

        by_spin = []
        for t in range(4):
            sums = [[None] * 4 for _ in range(2)]
            for i in range(3):
                for k in range(3):
                    first = [[entry(0, part, 3 * s + i, 3 * t + k) for part in range(2)] for s in range(4)]
                    second = [[entry(1, part, 3 * s + i, 3 * right_pair[t] + k) for part in range(2)] for s in range(4)]
                    for side, pair in enumerate((REVERSED, SWAPPED)):
                        for s in range(4):
                            ar, ai = first[pair[s]]
                            br, bi = second[s]
                            re = ar * br + ai * bi
                            im = ai * br - ar * bi
                            if sums[side][s] is None:
                                sums[side][s] = [re, im]
                            else:
                                sums[side][s] = [sums[side][s][0] + re, sums[side][s][1] + im]
            left = []
            for part in range(2):
                p0, p1, p2, p3 = [sums[0][s][part] for s in range(4)]
                even, odd = p0 + p2, p1 + p3
                q0, q1, q2, q3 = [sums[1][s][part] for s in range(4)]
                outer, inner = q0 - q3, q1 - q2
                left.append([even + odd, even - odd, outer - inner, outer + inner])
            by_spin.append(left)
        for mu in range(4):
            for part in range(2):
                p0, p1, p2, p3 = [by_spin[t][part][mu] for t in range(4)]
                if chunk == 0:
                    even, odd = p0 + p2, p1 + p3
                    pair = (even + odd, even - odd)
                else:
                    outer, inner = p0 - p3, p1 - p2
                    pair = (outer - inner, outer + inner)
                for side in range(2):
                    row = ((2 * mu + side) * 2 + part) * 8
                    fields[pl.ds(pl.multiple_of(h * 128, 128) + row, 8), :] = pair[side]
        return carry

    lax.fori_loop(0, 2, one_plane, 0)


def plane_transform(chunk, fields, fold_ref, twiddle_ref, plane_ref, put):
    high, low = split_values(fields[...])
    folded = dot(fold_ref[chunk], jnp.concatenate([high, low], axis=1))
    folded = folded[:256, :128] + folded[:256, 128:] + folded[256:, :128]
    halves = []
    for parity in range(2):
        re = folded[parity * 128 : parity * 128 + 64].reshape(4, 2, 8, 128)
        im = folded[parity * 128 + 64 : parity * 128 + 128].reshape(4, 2, 8, 128)
        cosines = twiddle_ref[0, parity * 32 : parity * 32 + 32, :].reshape(4, 1, 8, 128)
        sines = twiddle_ref[1, parity * 32 : parity * 32 + 32, :].reshape(4, 1, 8, 128)
        turned = jnp.concatenate(
            [(re * cosines + im * sines).reshape(64, 128), (im * cosines - re * sines).reshape(64, 128)], axis=1
        )
        halves.append(wide_dot(turned, plane_ref[parity, 0], plane_ref[parity, 1]))
    even_slot = (lax.broadcasted_iota(jnp.int32, (64, 128), 1) // 32) % 2 == 0
    for tile in range(2):
        a = halves[0][:, tile * 128 : (tile + 1) * 128]
        b = halves[1][:, tile * 128 : (tile + 1) * 128]
        put(2 * tile, jnp.where(even_slot, a, b))
        put(2 * tile + 1, jnp.where(even_slot, b, a))


def field_kernel(
    one_ref, two_ref, fold_hbm, twiddle_hbm, plane_hbm, out_ref, staged, sites, fields, fold_ref, twiddle_ref, plane_ref, sems
):
    copies = []
    for chunk in range(8):
        rows = 36 * PITCH
        source = (one_ref, two_ref)[chunk // 4]
        copies.append(
            pltpu.make_async_copy(
                source.at[pl.ds((chunk % 4) * rows, rows)], staged.at[pl.ds(chunk * rows, rows)], sems.at[chunk]
            )
        )
        copies[-1].start()
    tables = [
        pltpu.make_async_copy(source, target, sems.at[8 + index])
        for index, (source, target) in enumerate(
            ((fold_hbm, fold_ref), (twiddle_hbm, twiddle_ref), (plane_hbm, plane_ref))
        )
    ]
    for table in tables:
        table.start()
    for chunk in range(8):
        copies[chunk].wait()
        widen(chunk, staged, sites)
    for chunk in range(2):
        contract_half(chunk, sites, fields)
        if chunk == 0:
            for table in tables:
                table.wait()

        def put(kh, rows):
            out_ref[chunk, 4 * kh : 4 * kh + 4] = rows.reshape(4, 16, 128)

        plane_transform(chunk, fields, fold_ref, twiddle_ref, plane_ref, put)


def line_transform(held, flip, line_ref, staging, chunk):
    turned = []
    for g in range(2):
        block = jnp.concatenate([held[chunk, pl.ds(4 * g + f4, 32, stride=8), :] for f4 in range(4)], axis=0)
        across = block.T
        turned.append(jnp.concatenate([across[:64], across[64:]], axis=1))
    result = wide_dot(jnp.concatenate(turned, axis=0), line_ref[0], line_ref[1])
    lane = lax.broadcasted_iota(jnp.int32, (8, 128), 1)
    low_half, even_slot = lane < 64, (lane // 32) % 2 == 0
    for g in range(2):
        for k in range(2):
            for part in range(2):
                v = [
                    result[((g * 2 + k) * 4 + j) * 8 : ((g * 2 + k) * 4 + j + 1) * 8, part * 128 : (part + 1) * 128]
                    for j in range(4)
                ]
                w = [None] * 4
                for j in range(2):
                    w[j] = jnp.where(low_half, v[j], pltpu.roll(v[j + 2], 64, 1))
                    w[j + 2] = jnp.where(low_half, pltpu.roll(v[j], 64, 1), v[j + 2])
                for j in (0, 2):
                    first = jnp.where(even_slot, w[j], pltpu.roll(w[j + 1], 32, 1))
                    second = jnp.where(even_slot, pltpu.roll(w[j], 96, 1), w[j + 1])
                    start = pl.multiple_of(16 * lax.rem(k + flip, 2), 16) + part
                    staging[8 * chunk + 4 * g + j, pl.ds(start, 8, stride=2), :] = first
                    staging[8 * chunk + 4 * g + j + 1, pl.ds(start, 8, stride=2), :] = second


def exchange_kernel(fields_ref, line_ref, out_ref, held, staging, send_sems, recv_sems, last_send, last_recv, own_sems):
    ta, me = lax.axis_index("ta"), lax.axis_index("xyz")
    barrier = pltpu.get_barrier_semaphore()

    def greet(offset, carry):
        pl.semaphore_signal(
            barrier, inc=1, device_id={"xyz": lax.rem(me + offset, 16)}, device_id_type=MESH
        )
        pl.semaphore_signal(
            barrier, inc=1, device_id={"ta": lax.rem(ta + offset, 16)}, device_id_type=MESH
        )
        return carry

    lax.fori_loop(1, 16, greet, 0)
    pl.semaphore_wait(barrier, 30)

    def crossing(chunk, source, target, peer):
        return pltpu.make_async_remote_copy(
            src_ref=fields_ref.at[chunk, target],
            dst_ref=held.at[chunk, pl.ds(pl.multiple_of(source * 16, 16), 16)],
            send_sem=send_sems.at[chunk, target],
            recv_sem=recv_sems.at[chunk, source],
            device_id={"xyz": peer},
            device_id_type=MESH,
        )

    for chunk in range(2):

        def send(offset, carry, chunk=chunk):
            q = lax.rem(me + offset, 16)
            crossing(chunk, me, q, q).start()
            return carry

        lax.fori_loop(1, 16, send, 0)
        held[chunk, pl.ds(pl.multiple_of(me * 16, 16), 16), :] = fields_ref[chunk, me]

    flip = lax.rem(me // 4, 2)

    def leaving(f, f16, source):
        return pltpu.make_async_remote_copy(
            src_ref=staging.at[f16],
            dst_ref=out_ref.at[source],
            send_sem=last_send.at[f16],
            recv_sem=last_recv.at[source],
            device_id={"ta": f},
            device_id_type=MESH,
        )

    for chunk in range(2):

        def arrive(offset, carry, chunk=chunk):
            q = lax.rem(me + offset, 16)
            crossing(chunk, q, me, q).wait_recv()
            return carry

        lax.fori_loop(1, 16, arrive, 0)
        line_transform(held, flip, line_ref, staging, chunk)
        for f8 in range(8):
            f = 4 * (f8 // 2) + 2 * chunk + f8 % 2

            @pl.when(f != ta)
            def _(f=f, f16=8 * chunk + f8):
                leaving(f, f16, ta).start()

            @pl.when(f == ta)
            def _(f16=8 * chunk + f8):
                pltpu.make_async_copy(staging.at[f16], out_ref.at[ta], own_sems.at[0]).start()

    for chunk in range(2):

        def sent(offset, carry, chunk=chunk):
            q = lax.rem(me + offset, 16)
            crossing(chunk, me, q, q).wait_send()
            return carry

        lax.fori_loop(1, 16, sent, 0)
        for f8 in range(8):
            f = 4 * (f8 // 2) + 2 * chunk + f8 % 2

            @pl.when(f != ta)
            def _(f=f, f16=8 * chunk + f8):
                leaving(f, f16, ta).wait_send()

    pltpu.make_async_copy(staging.at[0], out_ref.at[ta], own_sems.at[0]).wait()

    def final(offset, carry):
        t = lax.rem(ta + offset, 16)
        leaving(t, 0, t).wait_recv()
        return carry

    lax.fori_loop(1, 16, final, 0)


def site_rows(prop):
    entries = prop.transpose(0, 2, 3, 1, 4).reshape(ENTRIES, 2, 16, 128)
    return entries.transpose(0, 2, 1, 3).reshape(ENTRIES * PITCH, 128)


def on_device(prop_one, prop_two):
    vmem, anywhere = pl.BlockSpec(memory_space=pltpu.VMEM), pl.BlockSpec(memory_space=pl.ANY)
    fields = pl.pallas_call(
        field_kernel,
        name="fields",
        out_shape=jax.ShapeDtypeStruct((2, 16, 16, 128), jnp.float32),
        in_specs=[anywhere] * 5,
        out_specs=vmem,
        scratch_shapes=[
            pltpu.VMEM((2 * ENTRIES * PITCH, 128), jnp.bfloat16),
            pltpu.VMEM((2 * ENTRIES * PITCH, 128), jnp.float32),
            pltpu.VMEM((256, 128), jnp.float32),
            pltpu.VMEM((2, 512, 256), jnp.bfloat16),
            pltpu.VMEM((2, 64, 128), jnp.float32),
            pltpu.VMEM((2, 2, 256, 256), jnp.bfloat16),
            pltpu.SemaphoreType.DMA((11,)),
        ],
        compiler_params=pltpu.CompilerParams(vmem_limit_bytes=67_043_328),
        cost_estimate=pl.CostEstimate(flops=20_000_000, bytes_accessed=4_000_000, transcendentals=0),
    )(site_rows(prop_one), site_rows(prop_two), jnp.asarray(fold_tables()), jnp.asarray(twiddle_tables()), jnp.asarray(plane_tables()))
    rows = pl.pallas_call(
        exchange_kernel,
        name="exchange",
        out_shape=jax.ShapeDtypeStruct((16, 32, 128), jnp.float32),
        in_specs=[vmem, vmem],
        out_specs=anywhere,
        scratch_shapes=[
            pltpu.VMEM((2, 256, 128), jnp.float32),
            pltpu.VMEM((16, 32, 128), jnp.float32),
            pltpu.SemaphoreType.DMA((2, 16)),
            pltpu.SemaphoreType.DMA((2, 16)),
            pltpu.SemaphoreType.DMA((16,)),
            pltpu.SemaphoreType.DMA((16,)),
            pltpu.SemaphoreType.DMA((1,)),
        ],
        compiler_params=pltpu.CompilerParams(collective_id=0, has_side_effects=True, vmem_limit_bytes=16 << 20),
    )(fields, jnp.asarray(line_tables()))
    return rows.reshape(16, 16, 2, 128).transpose(0, 2, 1, 3).reshape(16, 1, 2, 2048)


def solution(mesh):
    placed = (P("ta", None, None, None, "xyz"), P("ta", None, None, None, "xyz"))
    return jax.shard_map(
        on_device, mesh=mesh, in_specs=placed, out_specs=P(None, "ta", None, "xyz"), check_vma=False
    )
```

```python
import functools

import jax
import jax.numpy as jnp
import numpy as np
from jax import lax
from jax.experimental import pallas as pl
from jax.experimental.pallas import tpu as pltpu
from jax.sharding import PartitionSpec as P

L = 32
MESH = pl.DeviceIdType.MESH
ENTRIES = 144
FLAGS = {}
PITCH = 32

REVERSED = [3, 2, 1, 0]
SWAPPED = [2, 3, 0, 1]
LEFT_PHASE = [1j, -1.0, 1j, 1.0]
RIGHT_PHASE = [-1j, 1.0, -1j, -1.0]


def split_table(values):
    high = jnp.asarray(values, jnp.float32).astype(jnp.bfloat16)
    high_np = np.asarray(values, np.float32).astype(jnp.bfloat16).astype(np.float64)
    low = np.asarray(values - high_np, np.float32).astype(jnp.bfloat16)
    high = np.asarray(values, np.float32).astype(jnp.bfloat16)
    return high, low


def real_form(z):
    return np.stack([np.stack([z.real, -z.imag]), np.stack([z.imag, z.real])])


def fold_tables():
    result = []
    for chunk in range(2):
        table = np.zeros((2, 2, 4, 2, 8, 2, 8, 2, 8))
        for f8 in range(8):
            mu, nu = f8 // 2, 2 * chunk + f8 % 2
            phase = LEFT_PHASE[mu] * RIGHT_PHASE[nu]
            for parity in range(2):
                for m in range(4):
                    z = phase * np.exp(-2j * np.pi * np.arange(8) * (2 * m + parity) / 8)
                    form = real_form(z)
                    for x in range(2):
                        table[parity, :, m, x, f8, x, f8] = form
        result.append(np.concatenate(split_table(table.reshape(256, 256)), axis=0))
    return np.stack(result)


def twiddle_tables():
    kl = (2 * np.arange(4)[None, :] + np.arange(2)[:, None]).reshape(8)
    angle = 2 * np.pi * kl[:, None] * np.repeat(np.arange(4), 32)[None, :] / 32
    rows = np.stack([np.cos(angle), np.sin(angle)])
    return np.repeat(rows[:, :, None, :], 8, axis=2).reshape(2, 64, 128).astype(np.float32)


def plane_tables():
    yl, z = np.arange(4)[:, None], np.arange(32)[None, :]
    kz = np.array([4 * high + low for low in range(4) for high in range(8)])
    result = []
    for parity in range(2):
        table = np.zeros((2, 128, 2, 4, 32))
        for tile in range(2):
            for slot in range(4):
                part, kh = slot // 2, 2 * tile + (slot % 2 if parity == 0 else 1 - slot % 2)
                w = np.exp(-2j * np.pi * ((yl * kh / 4)[:, :, None] + z[:, :, None] * kz[None, None, :] / 32)) / 32
                form = real_form(w.reshape(128, 32))
                table[:, :, tile, slot] = form[part]
        result.append(np.stack(split_table(table.reshape(256, 256))))
    return np.stack(result)


def line_tables():
    w = np.exp(-2j * np.pi * np.arange(32)[:, None] * np.arange(32)[None, :] / 32) / np.sqrt(32)
    form = real_form(w)
    table = np.zeros((2, 4, 32, 2, 4, 32))
    for f4 in range(4):
        table[:, f4, :, :, f4] = form.transpose(1, 2, 0, 3)
    return np.stack(split_table(table.reshape(256, 256)))


def split_values(values):
    high = values.astype(jnp.bfloat16)
    low = (values - high.astype(jnp.float32)).astype(jnp.bfloat16)
    return high, low


def dot(a, b):
    return jnp.dot(a, b, preferred_element_type=jnp.float32)


def wide_dot(values, high_table, low_table):
    rows = values.shape[0]
    high, low = split_values(values)
    both = dot(jnp.concatenate([high, low], axis=0), high_table)
    return both[:rows] + both[rows:] + dot(high, low_table)


def widen(chunk, staged, sites):
    rows = 36 * PITCH
    base = chunk * rows

    def one(index, carry):
        start = pl.multiple_of(base + index * 128, 128)
        sites[pl.ds(start, 128), :] = staged[pl.ds(start, 128), :].astype(jnp.float32)
        return carry

    lax.fori_loop(0, rows // 128, one, 0)


def contract_half(chunk, sites, fields):
    right_pair = [REVERSED, SWAPPED][chunk]

    def one_plane(h, carry):
        def entry(prop, part, row, column):
            start = (prop * ENTRIES + row * 12 + column) * PITCH + part
            return sites[pl.ds(start + 16 * h, 8, stride=2), :]

        by_spin = []
        for t in range(4):
            sums = [[None] * 4 for _ in range(2)]
            for i in range(3):
                for k in range(3):
                    first = [[entry(0, part, 3 * s + i, 3 * t + k) for part in range(2)] for s in range(4)]
                    second = [[entry(1, part, 3 * s + i, 3 * right_pair[t] + k) for part in range(2)] for s in range(4)]
                    for side, pair in enumerate((REVERSED, SWAPPED)):
                        for s in range(4):
                            ar, ai = first[pair[s]]
                            br, bi = second[s]
                            re = ar * br + ai * bi
                            im = ai * br - ar * bi
                            if sums[side][s] is None:
                                sums[side][s] = [re, im]
                            else:
                                sums[side][s] = [sums[side][s][0] + re, sums[side][s][1] + im]
            left = []
            for part in range(2):
                p0, p1, p2, p3 = [sums[0][s][part] for s in range(4)]
                even, odd = p0 + p2, p1 + p3
                q0, q1, q2, q3 = [sums[1][s][part] for s in range(4)]
                outer, inner = q0 - q3, q1 - q2
                left.append([even + odd, even - odd, outer - inner, outer + inner])
            by_spin.append(left)
        for mu in range(4):
            for part in range(2):
                p0, p1, p2, p3 = [by_spin[t][part][mu] for t in range(4)]
                if chunk == 0:
                    even, odd = p0 + p2, p1 + p3
                    pair = (even + odd, even - odd)
                else:
                    outer, inner = p0 - p3, p1 - p2
                    pair = (outer - inner, outer + inner)
                for side in range(2):
                    row = ((2 * mu + side) * 2 + part) * 8
                    fields[pl.ds(pl.multiple_of(h * 128, 128) + row, 8), :] = pair[side]
        return carry

    lax.fori_loop(0, 2, one_plane, 0)


def plane_transform(chunk, fields, fold_ref, twiddle_ref, plane_ref, put):
    high, low = split_values(fields[...])
    folded = dot(fold_ref[chunk], jnp.concatenate([high, low], axis=1))
    folded = folded[:256, :128] + folded[:256, 128:] + folded[256:, :128]
    halves = []
    for parity in range(2):
        re = folded[parity * 128 : parity * 128 + 64].reshape(4, 2, 8, 128)
        im = folded[parity * 128 + 64 : parity * 128 + 128].reshape(4, 2, 8, 128)
        cosines = twiddle_ref[0, parity * 32 : parity * 32 + 32, :].reshape(4, 1, 8, 128)
        sines = twiddle_ref[1, parity * 32 : parity * 32 + 32, :].reshape(4, 1, 8, 128)
        turned = jnp.concatenate(
            [(re * cosines + im * sines).reshape(64, 128), (im * cosines - re * sines).reshape(64, 128)], axis=1
        )
        halves.append(wide_dot(turned, plane_ref[parity, 0], plane_ref[parity, 1]))
    even_slot = (lax.broadcasted_iota(jnp.int32, (64, 128), 1) // 32) % 2 == 0
    for tile in range(2):
        a = halves[0][:, tile * 128 : (tile + 1) * 128]
        b = halves[1][:, tile * 128 : (tile + 1) * 128]
        put(2 * tile, jnp.where(even_slot, a, b))
        put(2 * tile + 1, jnp.where(even_slot, b, a))


def line_transform(held, flip, line_ref, staging, chunk):
    turned = []
    for g in range(2):
        block = jnp.concatenate([held[chunk, pl.ds(4 * g + f4, 32, stride=8), :] for f4 in range(4)], axis=0)
        across = block.T
        turned.append(jnp.concatenate([across[:64], across[64:]], axis=1))
    result = wide_dot(jnp.concatenate(turned, axis=0), line_ref[0], line_ref[1])
    lane = lax.broadcasted_iota(jnp.int32, (8, 128), 1)
    low_half, even_slot = lane < 64, (lane // 32) % 2 == 0
    for g in range(2):
        for k in range(2):
            for part in range(2):
                v = [
                    result[((g * 2 + k) * 4 + j) * 8 : ((g * 2 + k) * 4 + j + 1) * 8, part * 128 : (part + 1) * 128]
                    for j in range(4)
                ]
                w = [None] * 4
                for j in range(2):
                    w[j] = jnp.where(low_half, v[j], pltpu.roll(v[j + 2], 64, 1))
                    w[j + 2] = jnp.where(low_half, pltpu.roll(v[j], 64, 1), v[j + 2])
                for j in (0, 2):
                    first = jnp.where(even_slot, w[j], pltpu.roll(w[j + 1], 32, 1))
                    second = jnp.where(even_slot, pltpu.roll(w[j], 96, 1), w[j + 1])
                    start = pl.multiple_of(16 * lax.rem(k + flip, 2), 16) + part
                    staging[8 * chunk + 4 * g + j, pl.ds(start, 8, stride=2), :] = first
                    staging[8 * chunk + 4 * g + j + 1, pl.ds(start, 8, stride=2), :] = second


def whole_kernel(
    one_ref, two_ref, fold_hbm, twiddle_hbm, plane_hbm, line_hbm, out_ref,
    staged, sites, fields, outgoing, held, staging, fold_ref, twiddle_ref, plane_ref, line_ref,
    load_sems, send_sems, recv_sems, last_send, last_recv, own_sem,
):
    ta, me = lax.axis_index("ta"), lax.axis_index("xyz")
    copies = []
    for chunk in range(8):
        rows = 36 * PITCH
        source = (one_ref, two_ref)[chunk // 4]
        copies.append(
            pltpu.make_async_copy(
                source.at[pl.ds((chunk % 4) * rows, rows)], staged.at[pl.ds(chunk * rows, rows)], load_sems.at[chunk]
            )
        )
        copies[-1].start()
    tables = [
        pltpu.make_async_copy(source, target, load_sems.at[8 + index])
        for index, (source, target) in enumerate(
            ((fold_hbm, fold_ref), (twiddle_hbm, twiddle_ref), (plane_hbm, plane_ref), (line_hbm, line_ref))
        )
    ]
    for table in tables:
        table.start()

    barrier = pltpu.get_barrier_semaphore()

    def greet(offset, carry):
        pl.semaphore_signal(
            barrier, inc=1, device_id={"xyz": lax.rem(me + offset, 16)}, device_id_type=MESH
        )
        pl.semaphore_signal(
            barrier, inc=1, device_id={"ta": lax.rem(ta + offset, 16)}, device_id_type=MESH
        )
        return carry

    lax.fori_loop(1, 16, greet, 0)

    def crossing(chunk, source, target, peer):
        return pltpu.make_async_remote_copy(
            src_ref=outgoing.at[chunk, target],
            dst_ref=held.at[chunk, pl.ds(pl.multiple_of(source * 16, 16), 16)],
            send_sem=send_sems.at[chunk, target],
            recv_sem=recv_sems.at[chunk, source],
            device_id={"xyz": peer},
            device_id_type=MESH,
        )

    for chunk in range(8):
        copies[chunk].wait()
        widen(chunk, staged, sites)
    for chunk in range(2):
        contract_half(chunk, sites, fields)
        if chunk == 0:
            for table in tables:
                table.wait()

        def put(kh, rows, chunk=chunk):
            outgoing[chunk, 4 * kh : 4 * kh + 4] = rows.reshape(4, 16, 128)

        plane_transform(chunk, fields, fold_ref, twiddle_ref, plane_ref, put)
        if chunk == 0:
            pl.semaphore_wait(barrier, 30)

        def send(offset, carry, chunk=chunk):
            q = lax.rem(me + offset, 16)
            crossing(chunk, me, q, q).start()
            return carry

        lax.fori_loop(1, 16, send, 0)
        held[chunk, pl.ds(pl.multiple_of(me * 16, 16), 16), :] = outgoing[chunk, me]
    flip = lax.rem(me // 4, 2)

    def leaving(f, f16, source):
        return pltpu.make_async_remote_copy(
            src_ref=staging.at[f16],
            dst_ref=out_ref.at[source],
            send_sem=last_send.at[f16],
            recv_sem=last_recv.at[source],
            device_id={"ta": f},
            device_id_type=MESH,
        )

    for chunk in range(2):

        def arrive(offset, carry, chunk=chunk):
            q = lax.rem(me + offset, 16)
            crossing(chunk, q, me, q).wait_recv()
            return carry

        lax.fori_loop(1, 16, arrive, 0)
        line_transform(held, flip, line_ref, staging, chunk)
        for f8 in range(8):
            f = 4 * (f8 // 2) + 2 * chunk + f8 % 2

            @pl.when(f != ta)
            def _(f=f, f16=8 * chunk + f8):
                leaving(f, f16, ta).start()

            @pl.when(f == ta)
            def _(f16=8 * chunk + f8):
                pltpu.make_async_copy(staging.at[f16], out_ref.at[ta], own_sem.at[0]).start()

    for chunk in range(2):

        def sent(offset, carry, chunk=chunk):
            q = lax.rem(me + offset, 16)
            crossing(chunk, me, q, q).wait_send()
            return carry

        lax.fori_loop(1, 16, sent, 0)
        for f8 in range(8):
            f = 4 * (f8 // 2) + 2 * chunk + f8 % 2

            @pl.when(f != ta)
            def _(f=f, f16=8 * chunk + f8):
                leaving(f, f16, ta).wait_send()

    pltpu.make_async_copy(staging.at[0], out_ref.at[ta], own_sem.at[0]).wait()

    def final(offset, carry):
        t = lax.rem(ta + offset, 16)
        leaving(t, 0, t).wait_recv()
        return carry

    lax.fori_loop(1, 16, final, 0)


def site_rows(prop):
    entries = prop.transpose(0, 2, 3, 1, 4).reshape(ENTRIES, 2, 16, 128)
    return entries.transpose(0, 2, 1, 3).reshape(ENTRIES * PITCH, 128)


def on_device(prop_one, prop_two):
    anywhere = pl.BlockSpec(memory_space=pl.ANY)
    rows = pl.pallas_call(
        whole_kernel,
        name="whole",
        out_shape=jax.ShapeDtypeStruct((16, 32, 128), jnp.float32),
        in_specs=[anywhere] * 6,
        out_specs=anywhere,
        scratch_shapes=[
            pltpu.VMEM((2 * ENTRIES * PITCH, 128), jnp.bfloat16),
            pltpu.VMEM((2 * ENTRIES * PITCH, 128), jnp.float32),
            pltpu.VMEM((256, 128), jnp.float32),
            pltpu.VMEM((2, 16, 16, 128), jnp.float32),
            pltpu.VMEM((2, 256, 128), jnp.float32),
            pltpu.VMEM((16, 32, 128), jnp.float32),
            pltpu.VMEM((2, 512, 256), jnp.bfloat16),
            pltpu.VMEM((2, 64, 128), jnp.float32),
            pltpu.VMEM((2, 2, 256, 256), jnp.bfloat16),
            pltpu.VMEM((2, 256, 256), jnp.bfloat16),
            pltpu.SemaphoreType.DMA((12,)),
            pltpu.SemaphoreType.DMA((2, 16)),
            pltpu.SemaphoreType.DMA((2, 16)),
            pltpu.SemaphoreType.DMA((16,)),
            pltpu.SemaphoreType.DMA((16,)),
            pltpu.SemaphoreType.DMA((1,)),
        ],
        compiler_params=pltpu.CompilerParams(
            collective_id=0, has_side_effects=True, vmem_limit_bytes=67_043_328 - (300 << 10), flags=FLAGS
        ),
    )(
        site_rows(prop_one),
        site_rows(prop_two),
        jnp.asarray(fold_tables()),
        jnp.asarray(twiddle_tables()),
        jnp.asarray(plane_tables()),
        jnp.asarray(line_tables()),
    )
    return rows.reshape(16, 16, 2, 128).transpose(0, 2, 1, 3).reshape(16, 1, 2, 2048)


def solution(mesh):
    placed = (P("ta", None, None, None, "xyz"), P("ta", None, None, None, "xyz"))
    return jax.shard_map(
        on_device, mesh=mesh, in_specs=placed, out_specs=P(None, "ta", None, "xyz"), check_vma=False
    )
```

```python
import functools

import jax
import jax.numpy as jnp
import numpy as np
from jax import lax
from jax.experimental import pallas as pl
from jax.experimental.pallas import tpu as pltpu
from jax.sharding import PartitionSpec as P

L = 32
MESH = pl.DeviceIdType.MESH
ENTRIES = 144
FLAGS = {}
PITCH = 32

REVERSED = [3, 2, 1, 0]
SWAPPED = [2, 3, 0, 1]
LEFT_PHASE = [1j, -1.0, 1j, 1.0]
RIGHT_PHASE = [-1j, 1.0, -1j, -1.0]


def field_of(chunk, f4):
    return 4 * (2 * (chunk % 2) + f4 // 2) + 2 * (chunk // 2) + f4 % 2


def split_table(values):
    high = jnp.asarray(values, jnp.float32).astype(jnp.bfloat16)
    high_np = np.asarray(values, np.float32).astype(jnp.bfloat16).astype(np.float64)
    low = np.asarray(values - high_np, np.float32).astype(jnp.bfloat16)
    high = np.asarray(values, np.float32).astype(jnp.bfloat16)
    return high, low


def real_form(z):
    return np.stack([np.stack([z.real, -z.imag]), np.stack([z.imag, z.real])])


def fold_tables():
    result = []
    for chunk in range(4):
        table = np.zeros((2, 2, 4, 2, 4, 2, 4, 2, 8))
        for f4 in range(4):
            mu, nu = divmod(field_of(chunk, f4), 4)
            phase = LEFT_PHASE[mu] * RIGHT_PHASE[nu]
            for parity in range(2):
                for m in range(4):
                    z = phase * np.exp(-2j * np.pi * np.arange(8) * (2 * m + parity) / 8)
                    form = real_form(z)
                    for x in range(2):
                        table[parity, :, m, x, f4, x, f4] = form
        result.append(np.concatenate(split_table(table.reshape(128, 128)), axis=0))
    return np.stack(result)


def twiddle_tables():
    kl = (2 * np.arange(4)[None, :] + np.arange(2)[:, None]).reshape(8)
    angle = 2 * np.pi * kl[:, None] * np.repeat(np.arange(4), 32)[None, :] / 32
    rows = np.stack([np.cos(angle), np.sin(angle)])
    rows = np.repeat(rows[:, :, None, :], 8, axis=2).reshape(2, 64, 128).astype(np.float32)
    return np.concatenate([rows] * 8)


def plane_tables():
    yl, z = np.arange(4)[:, None], np.arange(32)[None, :]
    kz = np.array([4 * high + low for low in range(4) for high in range(8)])
    result = []
    for parity in range(2):
        table = np.zeros((2, 128, 2, 4, 32))
        for tile in range(2):
            for slot in range(4):
                part, kh = slot // 2, 2 * tile + (slot % 2 if parity == 0 else 1 - slot % 2)
                w = np.exp(-2j * np.pi * ((yl * kh / 4)[:, :, None] + z[:, :, None] * kz[None, None, :] / 32)) / 32
                form = real_form(w.reshape(128, 32))
                table[:, :, tile, slot] = form[part]
        result.append(np.stack(split_table(table.reshape(256, 256))))
    return np.stack(result)


def line_tables():
    w = np.exp(-2j * np.pi * np.arange(32)[:, None] * np.arange(32)[None, :] / 32) / np.sqrt(32)
    form = real_form(w)
    table = np.zeros((2, 4, 32, 2, 4, 32))
    for f4 in range(4):
        table[:, f4, :, :, f4] = form.transpose(1, 2, 0, 3)
    return np.stack(split_table(table.reshape(256, 256)))


def split_values(values):
    high = values.astype(jnp.bfloat16)
    low = (values - high.astype(jnp.float32)).astype(jnp.bfloat16)
    return high, low


def dot(a, b):
    return jnp.dot(a, b, preferred_element_type=jnp.float32)


def wide_dot(values, high_table, low_table):
    rows = values.shape[0]
    high, low = split_values(values)
    both = dot(jnp.concatenate([high, low], axis=0), high_table)
    return both[:rows] + both[rows:] + dot(high, low_table)


def widen(chunk, staged, sites):
    rows = 36 * PITCH
    base = chunk * rows

    def one(index, carry):
        start = pl.multiple_of(base + index * 128, 128)
        sites[pl.ds(start, 128), :] = staged[pl.ds(start, 128), :].astype(jnp.float32)
        return carry

    lax.fori_loop(0, rows // 128, one, 0)


def contract_chunk(chunk, sites, fields):
    left_pair = [REVERSED, SWAPPED][chunk % 2]
    right_pair = [REVERSED, SWAPPED][chunk // 2]

    def combine(reversed_pair, p):
        if reversed_pair:
            even, odd = p[0] + p[2], p[1] + p[3]
            return even + odd, even - odd
        outer, inner = p[0] - p[3], p[1] - p[2]
        return outer - inner, outer + inner

    def one_plane(h, carry):
        def entry(prop, part, row, column):
            start = (prop * ENTRIES + row * 12 + column) * PITCH + part
            return sites[pl.ds(start + 16 * h, 8, stride=2), :]

        by_spin = []
        for t in range(4):
            sums = [None] * 4
            for i in range(3):
                for k in range(3):
                    for s in range(4):
                        ar, ai = [entry(0, part, 3 * left_pair[s] + i, 3 * t + k) for part in range(2)]
                        br, bi = [entry(1, part, 3 * s + i, 3 * right_pair[t] + k) for part in range(2)]
                        re = ar * br + ai * bi
                        im = ai * br - ar * bi
                        sums[s] = [re, im] if sums[s] is None else [sums[s][0] + re, sums[s][1] + im]
            by_spin.append([combine(chunk % 2 == 0, [sums[s][part] for s in range(4)]) for part in range(2)])
        for side in range(2):
            for part in range(2):
                pair = combine(chunk // 2 == 0, [by_spin[t][part][side] for t in range(4)])
                for other in range(2):
                    row = ((2 * side + other) * 2 + part) * 8
                    fields[pl.ds(pl.multiple_of(h * 64, 64) + row, 8), :] = pair[other]
        return carry

    lax.fori_loop(0, 2, one_plane, 0)


def plane_transform(chunk, fields, fold_ref, twiddle_ref, plane_ref, put):
    high, low = split_values(fields[...])
    folded = dot(fold_ref[chunk], jnp.concatenate([high, low], axis=1))
    folded = folded[:128, :128] + folded[:128, 128:] + folded[128:, :128]
    halves = []
    for parity in range(2):
        re = folded[parity * 64 : parity * 64 + 32]
        im = folded[parity * 64 + 32 : parity * 64 + 64]
        cosines = twiddle_ref[0, parity * 32 : parity * 32 + 32, :]
        sines = twiddle_ref[1, parity * 32 : parity * 32 + 32, :]
        turned = jnp.concatenate([re * cosines + im * sines, im * cosines - re * sines], axis=1)
        halves.append(wide_dot(turned, plane_ref[parity, 0], plane_ref[parity, 1]))
    even_slot = (lax.broadcasted_iota(jnp.int32, (32, 128), 1) // 32) % 2 == 0
    for tile in range(2):
        a = halves[0][:, tile * 128 : (tile + 1) * 128]
        b = halves[1][:, tile * 128 : (tile + 1) * 128]
        put(2 * tile, jnp.where(even_slot, a, b))
        put(2 * tile + 1, jnp.where(even_slot, b, a))


def line_transform(held, flip, line_ref, staging, chunk):
    block = jnp.concatenate([held[chunk, pl.ds(f4, 32, stride=4), :] for f4 in range(4)], axis=0)
    across = block.T
    result = wide_dot(jnp.concatenate([across[:64], across[64:]], axis=1), line_ref[0], line_ref[1])
    lane = lax.broadcasted_iota(jnp.int32, (8, 128), 1)
    low_half, even_slot = lane < 64, (lane // 32) % 2 == 0
    for k in range(2):
        for part in range(2):
            v = [
                result[(k * 4 + j) * 8 : (k * 4 + j + 1) * 8, part * 128 : (part + 1) * 128]
                for j in range(4)
            ]
            w = [None] * 4
            for j in range(2):
                w[j] = jnp.where(low_half, v[j], pltpu.roll(v[j + 2], 64, 1))
                w[j + 2] = jnp.where(low_half, pltpu.roll(v[j], 64, 1), v[j + 2])
            for j in (0, 2):
                first = jnp.where(even_slot, w[j], pltpu.roll(w[j + 1], 32, 1))
                second = jnp.where(even_slot, pltpu.roll(w[j], 96, 1), w[j + 1])
                start = pl.multiple_of(16 * lax.rem(k + flip, 2), 16) + part
                staging[4 * chunk + j, pl.ds(start, 8, stride=2), :] = first
                staging[4 * chunk + j + 1, pl.ds(start, 8, stride=2), :] = second


def whole_kernel(
    one_ref, two_ref, fold_hbm, twiddle_hbm, plane_hbm, line_hbm, out_ref,
    staged, sites, fields, outgoing, held, staging, fold_ref, twiddle_ref, plane_ref, line_ref,
    load_sems, send_sems, recv_sems, last_send, last_recv, own_sem,
):
    ta, me = lax.axis_index("ta"), lax.axis_index("xyz")
    barrier = pltpu.get_barrier_semaphore()

    def peer(step, turn):
        offset = 4 + (1 - 2 * lax.rem(step, 2)) * ((step + 1) // 2)
        return 8 * lax.rem(me // 8 + turn, 2) + lax.rem(me + offset, 8)

    def to_peers(action):
        def one(step, carry):
            action(peer(step, 1))
            action(peer(step, 0))
            return carry

        lax.fori_loop(0, 7, one, 0)
        action(peer(7, 1))

    to_peers(lambda q: pl.semaphore_signal(barrier, inc=1, device_id={"xyz": q}, device_id_type=MESH))

    def greet(offset, carry):
        pl.semaphore_signal(
            barrier, inc=1, device_id={"ta": lax.rem(ta + offset, 16)}, device_id_type=MESH
        )
        return carry

    lax.fori_loop(1, 16, greet, 0)

    copies = []
    for part in range(8):
        rows = 36 * PITCH
        source = (one_ref, two_ref)[part // 4]
        copies.append(
            pltpu.make_async_copy(
                source.at[pl.ds((part % 4) * rows, rows)], staged.at[pl.ds(part * rows, rows)], load_sems.at[part]
            )
        )
        copies[-1].start()
    tables = [
        pltpu.make_async_copy(source, target, load_sems.at[8 + index])
        for index, (source, target) in enumerate(
            ((fold_hbm, fold_ref), (twiddle_hbm.at[0:2], twiddle_ref), (plane_hbm, plane_ref), (line_hbm, line_ref))
        )
    ]
    for table in tables:
        table.start()

    def crossing(chunk, source, target, peer):
        return pltpu.make_async_remote_copy(
            src_ref=outgoing.at[chunk, target],
            dst_ref=held.at[chunk, pl.ds(pl.multiple_of(source * 8, 8), 8)],
            send_sem=send_sems.at[chunk, target],
            recv_sem=recv_sems.at[chunk, source],
            device_id={"xyz": peer},
            device_id_type=MESH,
        )

    for part in range(8):
        copies[part].wait()
        widen(part, staged, sites)
    for chunk in range(4):
        contract_chunk(chunk, sites, fields)
        if chunk == 0:
            for table in tables:
                table.wait()

        def put(kh, rows, chunk=chunk):
            outgoing[chunk, 4 * kh : 4 * kh + 4] = rows.reshape(4, 8, 128)

        plane_transform(chunk, fields, fold_ref, twiddle_ref, plane_ref, put)
        if chunk == 0:
            pl.semaphore_wait(barrier, 30)
        to_peers(lambda q, chunk=chunk: crossing(chunk, me, q, q).start())
        held[chunk, pl.ds(pl.multiple_of(me * 8, 8), 8), :] = outgoing[chunk, me]

    flip = lax.rem(me // 4, 2)

    def leaving(f, slot, source):
        return pltpu.make_async_remote_copy(
            src_ref=staging.at[slot],
            dst_ref=out_ref.at[source],
            send_sem=last_send.at[slot],
            recv_sem=last_recv.at[source],
            device_id={"ta": f},
            device_id_type=MESH,
        )

    for chunk in range(4):

        def arrive(offset, carry, chunk=chunk):
            q = lax.rem(me + offset, 16)
            crossing(chunk, q, me, q).wait_recv()
            return carry

        lax.fori_loop(1, 16, arrive, 0)
        line_transform(held, flip, line_ref, staging, chunk)
        for f4 in range(4):
            f = field_of(chunk, f4)

            @pl.when(f != ta)
            def _(f=f, slot=4 * chunk + f4):
                leaving(f, slot, ta).start()

            @pl.when(f == ta)
            def _(slot=4 * chunk + f4):
                pltpu.make_async_copy(staging.at[slot], out_ref.at[ta], own_sem.at[0]).start()

    for chunk in range(4):

        def sent(offset, carry, chunk=chunk):
            q = lax.rem(me + offset, 16)
            crossing(chunk, me, q, q).wait_send()
            return carry

        lax.fori_loop(1, 16, sent, 0)
        for f4 in range(4):
            f = field_of(chunk, f4)

            @pl.when(f != ta)
            def _(f=f, slot=4 * chunk + f4):
                leaving(f, slot, ta).wait_send()

    pltpu.make_async_copy(staging.at[0], out_ref.at[ta], own_sem.at[0]).wait()

    def final(offset, carry):
        t = lax.rem(ta + offset, 16)
        leaving(t, 0, t).wait_recv()
        return carry

    lax.fori_loop(1, 16, final, 0)


def site_rows(prop):
    entries = prop.transpose(0, 2, 3, 1, 4).reshape(ENTRIES, 2, 16, 128)
    return entries.transpose(0, 2, 1, 3).reshape(ENTRIES * PITCH, 128)


def on_device(prop_one, prop_two):
    anywhere = pl.BlockSpec(memory_space=pl.ANY)
    rows = pl.pallas_call(
        whole_kernel,
        name="whole",
        out_shape=jax.ShapeDtypeStruct((16, 32, 128), jnp.float32),
        in_specs=[anywhere] * 6,
        out_specs=anywhere,
        scratch_shapes=[
            pltpu.VMEM((2 * ENTRIES * PITCH, 128), jnp.bfloat16),
            pltpu.VMEM((2 * ENTRIES * PITCH, 128), jnp.float32),
            pltpu.VMEM((128, 128), jnp.float32),
            pltpu.VMEM((4, 16, 8, 128), jnp.float32),
            pltpu.VMEM((4, 128, 128), jnp.float32),
            pltpu.VMEM((16, 32, 128), jnp.float32),
            pltpu.VMEM((4, 256, 128), jnp.bfloat16),
            pltpu.VMEM((2, 64, 128), jnp.float32),
            pltpu.VMEM((2, 2, 256, 256), jnp.bfloat16),
            pltpu.VMEM((2, 256, 256), jnp.bfloat16),
            pltpu.SemaphoreType.DMA((12,)),
            pltpu.SemaphoreType.DMA((4, 16)),
            pltpu.SemaphoreType.DMA((4, 16)),
            pltpu.SemaphoreType.DMA((16,)),
            pltpu.SemaphoreType.DMA((16,)),
            pltpu.SemaphoreType.DMA((1,)),
        ],
        compiler_params=pltpu.CompilerParams(
            collective_id=0, has_side_effects=True, vmem_limit_bytes=67_043_328 - (10650 << 10), flags=FLAGS
        ),
    )(
        site_rows(prop_one),
        site_rows(prop_two),
        jnp.asarray(fold_tables()),
        jnp.asarray(twiddle_tables()),
        jnp.asarray(plane_tables()),
        jnp.asarray(line_tables()),
    )
    return rows.reshape(16, 16, 2, 128).transpose(0, 2, 1, 3).reshape(16, 1, 2, 2048)


def solution(mesh):
    placed = (P("ta", None, None, None, "xyz"), P("ta", None, None, None, "xyz"))
    return jax.shard_map(
        on_device, mesh=mesh, in_specs=placed, out_specs=P(None, "ta", None, "xyz"), check_vma=False
    )
```

```python
import functools

import jax
import jax.numpy as jnp
import numpy as np
from jax import lax
from jax.experimental import pallas as pl
from jax.experimental.pallas import tpu as pltpu
from jax.sharding import PartitionSpec as P

L = 32
MESH = pl.DeviceIdType.MESH
ENTRIES = 144
FLAGS = {}
PITCH = 32

REVERSED = [3, 2, 1, 0]
SWAPPED = [2, 3, 0, 1]
LEFT_PHASE = [1j, -1.0, 1j, 1.0]
RIGHT_PHASE = [-1j, 1.0, -1j, -1.0]


def split_table(values):
    high = jnp.asarray(values, jnp.float32).astype(jnp.bfloat16)
    high_np = np.asarray(values, np.float32).astype(jnp.bfloat16).astype(np.float64)
    low = np.asarray(values - high_np, np.float32).astype(jnp.bfloat16)
    high = np.asarray(values, np.float32).astype(jnp.bfloat16)
    return high, low


def real_form(z):
    return np.stack([np.stack([z.real, -z.imag]), np.stack([z.imag, z.real])])


def fold_tables():
    result = []
    for chunk in range(2):
        table = np.zeros((2, 2, 4, 2, 8, 2, 8, 2, 8))
        for f8 in range(8):
            mu, nu = f8 // 2, 2 * chunk + f8 % 2
            phase = LEFT_PHASE[mu] * RIGHT_PHASE[nu]
            for parity in range(2):
                for m in range(4):
                    z = phase * np.exp(-2j * np.pi * np.arange(8) * (2 * m + parity) / 8)
                    form = real_form(z)
                    for x in range(2):
                        table[parity, :, m, x, f8, x, f8] = form
        result.append(np.concatenate(split_table(table.reshape(256, 256)), axis=0))
    return np.stack(result)


def twiddle_tables():
    kl = (2 * np.arange(4)[None, :] + np.arange(2)[:, None]).reshape(8)
    angle = 2 * np.pi * kl[:, None] * np.repeat(np.arange(4), 32)[None, :] / 32
    rows = np.stack([np.cos(angle), np.sin(angle)])
    rows = np.repeat(rows[:, :, None, :], 8, axis=2).reshape(2, 64, 128).astype(np.float32)
    return np.concatenate([rows] * 8)


def plane_tables():
    yl, z = np.arange(4)[:, None], np.arange(32)[None, :]
    kz = np.array([4 * high + low for low in range(4) for high in range(8)])
    result = []
    for parity in range(2):
        table = np.zeros((2, 128, 2, 4, 32))
        for tile in range(2):
            for slot in range(4):
                part, kh = slot // 2, 2 * tile + (slot % 2 if parity == 0 else 1 - slot % 2)
                w = np.exp(-2j * np.pi * ((yl * kh / 4)[:, :, None] + z[:, :, None] * kz[None, None, :] / 32)) / 32
                form = real_form(w.reshape(128, 32))
                table[:, :, tile, slot] = form[part]
        result.append(np.stack(split_table(table.reshape(256, 256))))
    return np.stack(result)


def line_tables():
    w = np.exp(-2j * np.pi * np.arange(32)[:, None] * np.arange(32)[None, :] / 32) / np.sqrt(32)
    form = real_form(w)
    table = np.zeros((2, 4, 32, 2, 4, 32))
    for f4 in range(4):
        table[:, f4, :, :, f4] = form.transpose(1, 2, 0, 3)
    return np.stack(split_table(table.reshape(256, 256)))


def split_values(values):
    high = values.astype(jnp.bfloat16)
    low = (values - high.astype(jnp.float32)).astype(jnp.bfloat16)
    return high, low


def dot(a, b):
    return jnp.dot(a, b, preferred_element_type=jnp.float32)


def wide_dot(values, high_table, low_table):
    rows = values.shape[0]
    high, low = split_values(values)
    both = dot(jnp.concatenate([high, low], axis=0), high_table)
    return both[:rows] + both[rows:] + dot(high, low_table)


def widen(chunk, staged, sites):
    rows = 36 * PITCH
    base = chunk * rows

    def one(index, carry):
        start = pl.multiple_of(base + index * 128, 128)
        sites[pl.ds(start, 128), :] = staged[pl.ds(start, 128), :].astype(jnp.float32)
        return carry

    lax.fori_loop(0, rows // 128, one, 0)


def combine(reversed_pair, p):
    if reversed_pair:
        even, odd = p[0] + p[2], p[1] + p[3]
        return even + odd, even - odd
    outer, inner = p[0] - p[3], p[1] - p[2]
    return outer - inner, outer + inner


def contract_half(half, sites, spins, fields):
    def one_spin(index, carry):
        h, t = index // 4, lax.rem(index, 4)
        paired = 3 - t if half == 0 else lax.rem(t + 2, 4)
        first_base = pl.multiple_of(16 * h + 3 * PITCH * t, 16)
        second_base = pl.multiple_of(16 * h + 3 * PITCH * paired, 16)

        def entry(prop, part, row, k):
            start = (prop * ENTRIES + row * 12 + k) * PITCH + part
            return sites[pl.ds((first_base, second_base)[prop] + start, 8, stride=2), :]

        sums = [[None] * 4 for _ in range(2)]
        for i in range(3):
            for k in range(3):
                first = [[entry(0, part, 3 * s + i, k) for part in range(2)] for s in range(4)]
                second = [[entry(1, part, 3 * s + i, k) for part in range(2)] for s in range(4)]
                for s in range(4):
                    for side, pair in enumerate((REVERSED, SWAPPED)):
                        ar, ai = first[pair[s]]
                        br, bi = second[s]
                        re = ar * br + ai * bi
                        im = ai * br - ar * bi
                        old = sums[side][s]
                        sums[side][s] = [re, im] if old is None else [old[0] + re, old[1] + im]
        for side in range(2):
            for part in range(2):
                pair = combine(side == 0, [sums[side][s][part] for s in range(4)])
                for other in range(2):
                    spins[index, 4 * side + 2 * other + part] = pair[other]
        return carry

    lax.fori_loop(0, 8, one_spin, 0)
    for h in range(2):
        for side in range(2):
            for left in range(2):
                for part in range(2):
                    pair = combine(half == 0, [spins[4 * h + t, 4 * side + 2 * left + part] for t in range(4)])
                    for other in range(2):
                        row = h * 128 + ((2 * (2 * side + left) + other) * 2 + part) * 8
                        fields[row : row + 8, :] = pair[other]


def plane_transform(chunk, fields, fold_ref, twiddle_ref, plane_ref, put):
    high, low = split_values(fields[...])
    folded = dot(fold_ref[chunk], jnp.concatenate([high, low], axis=1))
    folded = folded[:256, :128] + folded[:256, 128:] + folded[256:, :128]
    halves = []
    for parity in range(2):
        re = folded[parity * 128 : parity * 128 + 64].reshape(4, 2, 8, 128)
        im = folded[parity * 128 + 64 : parity * 128 + 128].reshape(4, 2, 8, 128)
        cosines = twiddle_ref[0, parity * 32 : parity * 32 + 32, :].reshape(4, 1, 8, 128)
        sines = twiddle_ref[1, parity * 32 : parity * 32 + 32, :].reshape(4, 1, 8, 128)
        turned = jnp.concatenate(
            [(re * cosines + im * sines).reshape(64, 128), (im * cosines - re * sines).reshape(64, 128)], axis=1
        )
        halves.append(wide_dot(turned, plane_ref[parity, 0], plane_ref[parity, 1]))
    even_slot = (lax.broadcasted_iota(jnp.int32, (64, 128), 1) // 32) % 2 == 0
    for tile in range(2):
        a = halves[0][:, tile * 128 : (tile + 1) * 128]
        b = halves[1][:, tile * 128 : (tile + 1) * 128]
        put(2 * tile, jnp.where(even_slot, a, b))
        put(2 * tile + 1, jnp.where(even_slot, b, a))


def line_transform(held, flip, line_ref, staging, chunk):
    turned = []
    for g in range(2):
        block = jnp.concatenate([held[chunk, pl.ds(4 * g + f4, 32, stride=8), :] for f4 in range(4)], axis=0)
        across = block.T
        turned.append(jnp.concatenate([across[:64], across[64:]], axis=1))
    result = wide_dot(jnp.concatenate(turned, axis=0), line_ref[0], line_ref[1])
    lane = lax.broadcasted_iota(jnp.int32, (8, 128), 1)
    low_half, even_slot = lane < 64, (lane // 32) % 2 == 0
    for g in range(2):
        for k in range(2):
            for part in range(2):
                v = [
                    result[((g * 2 + k) * 4 + j) * 8 : ((g * 2 + k) * 4 + j + 1) * 8, part * 128 : (part + 1) * 128]
                    for j in range(4)
                ]
                w = [None] * 4
                for j in range(2):
                    w[j] = jnp.where(low_half, v[j], pltpu.roll(v[j + 2], 64, 1))
                    w[j + 2] = jnp.where(low_half, pltpu.roll(v[j], 64, 1), v[j + 2])
                for j in (0, 2):
                    first = jnp.where(even_slot, w[j], pltpu.roll(w[j + 1], 32, 1))
                    second = jnp.where(even_slot, pltpu.roll(w[j], 96, 1), w[j + 1])
                    start = pl.multiple_of(16 * lax.rem(k + flip, 2), 16) + part
                    staging[8 * chunk + 4 * g + j, pl.ds(start, 8, stride=2), :] = first
                    staging[8 * chunk + 4 * g + j + 1, pl.ds(start, 8, stride=2), :] = second


def whole_kernel(
    one_ref, two_ref, fold_hbm, twiddle_hbm, plane_hbm, line_hbm, out_ref,
    staged, sites, spins, fields, outgoing, held, staging, fold_ref, twiddle_ref, plane_ref, line_ref,
    load_sems, send_sems, recv_sems, last_send, last_recv, own_sem,
):
    ta, me = lax.axis_index("ta"), lax.axis_index("xyz")
    barrier = pltpu.get_barrier_semaphore()

    def to_peers(action):
        def one(step, carry):
            turn, near = 1 - step // 8, lax.rem(step, 8)
            offset = 4 + (1 - 2 * lax.rem(near, 2)) * ((near + 1) // 2)
            action(8 * lax.rem(me // 8 + turn, 2) + lax.rem(me + offset, 8))
            return carry

        lax.fori_loop(0, 15, one, 0)

    to_peers(lambda q: pl.semaphore_signal(barrier, inc=1, device_id={"xyz": q}, device_id_type=MESH))

    def greet(offset, carry):
        pl.semaphore_signal(
            barrier, inc=1, device_id={"ta": lax.rem(ta + offset, 16)}, device_id_type=MESH
        )
        return carry

    lax.fori_loop(1, 16, greet, 0)

    copies = []
    for chunk in range(8):
        rows = 36 * PITCH
        source = (one_ref, two_ref)[chunk // 4]
        copies.append(
            pltpu.make_async_copy(
                source.at[pl.ds((chunk % 4) * rows, rows)], staged.at[pl.ds(chunk * rows, rows)], load_sems.at[chunk]
            )
        )
        copies[-1].start()
    tables = [
        pltpu.make_async_copy(source, target, load_sems.at[8 + index])
        for index, (source, target) in enumerate(
            ((fold_hbm, fold_ref), (twiddle_hbm.at[0:2], twiddle_ref), (plane_hbm, plane_ref), (line_hbm, line_ref))
        )
    ]
    for table in tables:
        table.start()

    def crossing(chunk, source, target, peer):
        return pltpu.make_async_remote_copy(
            src_ref=outgoing.at[chunk, target],
            dst_ref=held.at[chunk, pl.ds(pl.multiple_of(source * 16, 16), 16)],
            send_sem=send_sems.at[chunk, target],
            recv_sem=recv_sems.at[chunk, source],
            device_id={"xyz": peer},
            device_id_type=MESH,
        )

    for chunk in range(8):
        copies[chunk].wait()
        widen(chunk, staged, sites)
    for chunk in range(2):
        contract_half(chunk, sites, spins, fields)
        if chunk == 0:
            for table in tables:
                table.wait()

        def put(kh, rows, chunk=chunk):
            outgoing[chunk, 4 * kh : 4 * kh + 4] = rows.reshape(4, 16, 128)

        plane_transform(chunk, fields, fold_ref, twiddle_ref, plane_ref, put)
        if chunk == 0:
            pl.semaphore_wait(barrier, 30)

        to_peers(lambda q, chunk=chunk: crossing(chunk, me, q, q).start())
        held[chunk, pl.ds(pl.multiple_of(me * 16, 16), 16), :] = outgoing[chunk, me]
    flip = lax.rem(me // 4, 2)

    def leaving(f, f16, source):
        return pltpu.make_async_remote_copy(
            src_ref=staging.at[f16],
            dst_ref=out_ref.at[source],
            send_sem=last_send.at[f16],
            recv_sem=last_recv.at[source],
            device_id={"ta": f},
            device_id_type=MESH,
        )

    for chunk in range(2):

        def arrive(offset, carry, chunk=chunk):
            q = lax.rem(me + offset, 16)
            crossing(chunk, q, me, q).wait_recv()
            return carry

        lax.fori_loop(1, 16, arrive, 0)
        line_transform(held, flip, line_ref, staging, chunk)
        for f8 in range(8):
            f = 4 * (f8 // 2) + 2 * chunk + f8 % 2

            @pl.when(f != ta)
            def _(f=f, f16=8 * chunk + f8):
                leaving(f, f16, ta).start()

            @pl.when(f == ta)
            def _(f16=8 * chunk + f8):
                pltpu.make_async_copy(staging.at[f16], out_ref.at[ta], own_sem.at[0]).start()

    for chunk in range(2):

        def sent(offset, carry, chunk=chunk):
            q = lax.rem(me + offset, 16)
            crossing(chunk, me, q, q).wait_send()
            return carry

        lax.fori_loop(1, 16, sent, 0)
        for f8 in range(8):
            f = 4 * (f8 // 2) + 2 * chunk + f8 % 2

            @pl.when(f != ta)
            def _(f=f, f16=8 * chunk + f8):
                leaving(f, f16, ta).wait_send()

    pltpu.make_async_copy(staging.at[0], out_ref.at[ta], own_sem.at[0]).wait()

    def final(offset, carry):
        t = lax.rem(ta + offset, 16)
        leaving(t, 0, t).wait_recv()
        return carry

    lax.fori_loop(1, 16, final, 0)


def site_rows(prop):
    entries = prop.transpose(0, 2, 3, 1, 4).reshape(ENTRIES, 2, 16, 128)
    return entries.transpose(0, 2, 1, 3).reshape(ENTRIES * PITCH, 128)


def on_device(prop_one, prop_two):
    anywhere = pl.BlockSpec(memory_space=pl.ANY)
    rows = pl.pallas_call(
        whole_kernel,
        name="whole",
        out_shape=jax.ShapeDtypeStruct((16, 32, 128), jnp.float32),
        in_specs=[anywhere] * 6,
        out_specs=anywhere,
        scratch_shapes=[
            pltpu.VMEM((2 * ENTRIES * PITCH, 128), jnp.bfloat16),
            pltpu.VMEM((2 * ENTRIES * PITCH, 128), jnp.float32),
            pltpu.VMEM((8, 8, 8, 128), jnp.float32),
            pltpu.VMEM((256, 128), jnp.float32),
            pltpu.VMEM((2, 16, 16, 128), jnp.float32),
            pltpu.VMEM((2, 256, 128), jnp.float32),
            pltpu.VMEM((16, 32, 128), jnp.float32),
            pltpu.VMEM((2, 512, 256), jnp.bfloat16),
            pltpu.VMEM((2, 64, 128), jnp.float32),
            pltpu.VMEM((2, 2, 256, 256), jnp.bfloat16),
            pltpu.VMEM((2, 256, 256), jnp.bfloat16),
            pltpu.SemaphoreType.DMA((12,)),
            pltpu.SemaphoreType.DMA((2, 16)),
            pltpu.SemaphoreType.DMA((2, 16)),
            pltpu.SemaphoreType.DMA((16,)),
            pltpu.SemaphoreType.DMA((16,)),
            pltpu.SemaphoreType.DMA((1,)),
        ],
        compiler_params=pltpu.CompilerParams(
            collective_id=0, has_side_effects=True, vmem_limit_bytes=67_043_328 - (10650 << 10), flags=FLAGS
        ),
    )(
        site_rows(prop_one),
        site_rows(prop_two),
        jnp.asarray(fold_tables()),
        jnp.asarray(twiddle_tables()),
        jnp.asarray(plane_tables()),
        jnp.asarray(line_tables()),
    )
    return rows.reshape(16, 16, 2, 128).transpose(0, 2, 1, 3).reshape(16, 1, 2, 2048)


def solution(mesh):
    placed = (P("ta", None, None, None, "xyz"), P("ta", None, None, None, "xyz"))
    return jax.shard_map(
        on_device, mesh=mesh, in_specs=placed, out_specs=P(None, "ta", None, "xyz"), check_vma=False
    )
```

```python
import functools

import jax
import jax.numpy as jnp
import numpy as np
from jax import lax
from jax.experimental import pallas as pl
from jax.experimental.pallas import tpu as pltpu
from jax.sharding import PartitionSpec as P

L = 32
MESH = pl.DeviceIdType.MESH
ENTRIES = 144
FLAGS = {}
PITCH = 32

REVERSED = [3, 2, 1, 0]
SWAPPED = [2, 3, 0, 1]
LEFT_PHASE = [1j, -1.0, 1j, 1.0]
RIGHT_PHASE = [-1j, 1.0, -1j, -1.0]


def split_table(values):
    high = jnp.asarray(values, jnp.float32).astype(jnp.bfloat16)
    high_np = np.asarray(values, np.float32).astype(jnp.bfloat16).astype(np.float64)
    low = np.asarray(values - high_np, np.float32).astype(jnp.bfloat16)
    high = np.asarray(values, np.float32).astype(jnp.bfloat16)
    return high, low


def real_form(z):
    return np.stack([np.stack([z.real, -z.imag]), np.stack([z.imag, z.real])])


def fold_tables():
    result = []
    for chunk in range(2):
        table = np.zeros((2, 2, 4, 2, 8, 2, 8, 2, 8))
        for f8 in range(8):
            mu, nu = f8 // 2, 2 * chunk + f8 % 2
            phase = LEFT_PHASE[mu] * RIGHT_PHASE[nu]
            for parity in range(2):
                for m in range(4):
                    z = phase * np.exp(-2j * np.pi * np.arange(8) * (2 * m + parity) / 8)
                    form = real_form(z)
                    for x in range(2):
                        table[parity, :, m, x, f8, x, f8] = form
        result.append(np.concatenate(split_table(table.reshape(256, 256)), axis=0))
    return np.stack(result)


def twiddle_tables():
    kl = (2 * np.arange(4)[None, :] + np.arange(2)[:, None]).reshape(8)
    angle = 2 * np.pi * kl[:, None] * np.repeat(np.arange(4), 32)[None, :] / 32
    rows = np.stack([np.cos(angle), np.sin(angle)])
    rows = np.repeat(rows[:, :, None, :], 8, axis=2).reshape(2, 64, 128).astype(np.float32)
    return np.concatenate([rows] * 8)


def plane_tables():
    yl, z = np.arange(4)[:, None], np.arange(32)[None, :]
    kz = np.array([4 * high + low for low in range(4) for high in range(8)])
    result = []
    for parity in range(2):
        table = np.zeros((2, 128, 2, 4, 32))
        for tile in range(2):
            for slot in range(4):
                part, kh = slot // 2, 2 * tile + (slot % 2 if parity == 0 else 1 - slot % 2)
                w = np.exp(-2j * np.pi * ((yl * kh / 4)[:, :, None] + z[:, :, None] * kz[None, None, :] / 32)) / 32
                form = real_form(w.reshape(128, 32))
                table[:, :, tile, slot] = form[part]
        result.append(np.stack(split_table(table.reshape(256, 256))))
    return np.stack(result)


def line_tables():
    w = np.exp(-2j * np.pi * np.arange(32)[:, None] * np.arange(32)[None, :] / 32) / np.sqrt(32)
    form = real_form(w)
    table = np.zeros((2, 4, 32, 2, 4, 32))
    for f4 in range(4):
        table[:, f4, :, :, f4] = form.transpose(1, 2, 0, 3)
    return np.stack(split_table(table.reshape(256, 256)))


def split_values(values):
    high = values.astype(jnp.bfloat16)
    low = (values - high.astype(jnp.float32)).astype(jnp.bfloat16)
    return high, low


def dot(a, b):
    return jnp.dot(a, b, preferred_element_type=jnp.float32)


def wide_dot(values, high_table, low_table):
    rows = values.shape[0]
    high, low = split_values(values)
    both = dot(jnp.concatenate([high, low], axis=0), high_table)
    return both[:rows] + both[rows:] + dot(high, low_table)


def widen(chunk, staged, sites):
    rows = 36 * PITCH
    base = chunk * rows

    def one(index, carry):
        start = pl.multiple_of(base + index * 384, 128)
        sites[pl.ds(start, 384), :] = staged[pl.ds(start, 384), :].astype(jnp.float32)
        return carry

    lax.fori_loop(0, rows // 384, one, 0)


def combine(reversed_pair, p):
    if reversed_pair:
        even, odd = p[0] + p[2], p[1] + p[3]
        return even + odd, even - odd
    outer, inner = p[0] - p[3], p[1] - p[2]
    return outer - inner, outer + inner


def contract_half(half, sites, spins, fields):
    def one_spin(index, carry):
        h, t = index // 4, lax.rem(index, 4)
        paired = 3 - t if half == 0 else lax.rem(t + 2, 4)
        first_base = pl.multiple_of(16 * h + 3 * PITCH * t, 16)
        second_base = pl.multiple_of(16 * h + 3 * PITCH * paired, 16)

        def entry(prop, part, row, k):
            start = (prop * ENTRIES + row * 12 + k) * PITCH + part
            return sites[pl.ds((first_base, second_base)[prop] + start, 8, stride=2), :]

        sums = [[None] * 4 for _ in range(2)]
        for i in range(3):
            for k in range(3):
                first = [[entry(0, part, 3 * s + i, k) for part in range(2)] for s in range(4)]
                second = [[entry(1, part, 3 * s + i, k) for part in range(2)] for s in range(4)]
                for s in range(4):
                    for side, pair in enumerate((REVERSED, SWAPPED)):
                        ar, ai = first[pair[s]]
                        br, bi = second[s]
                        re = ar * br + ai * bi
                        im = ai * br - ar * bi
                        old = sums[side][s]
                        sums[side][s] = [re, im] if old is None else [old[0] + re, old[1] + im]
        for side in range(2):
            for part in range(2):
                pair = combine(side == 0, [sums[side][s][part] for s in range(4)])
                for other in range(2):
                    spins[index, 4 * side + 2 * other + part] = pair[other]
        return carry

    lax.fori_loop(0, 8, one_spin, 0, unroll=2)
    for h in range(2):
        for side in range(2):
            for left in range(2):
                for part in range(2):
                    pair = combine(half == 0, [spins[4 * h + t, 4 * side + 2 * left + part] for t in range(4)])
                    for other in range(2):
                        row = h * 128 + ((2 * (2 * side + left) + other) * 2 + part) * 8
                        fields[row : row + 8, :] = pair[other]


def plane_transform(chunk, fields, fold_ref, twiddle_ref, plane_ref, put):
    high, low = split_values(fields[...])
    folded = dot(fold_ref[chunk], jnp.concatenate([high, low], axis=1))
    folded = folded[:256, :128] + folded[:256, 128:] + folded[256:, :128]
    halves = []
    for parity in range(2):
        re = folded[parity * 128 : parity * 128 + 64].reshape(4, 2, 8, 128)
        im = folded[parity * 128 + 64 : parity * 128 + 128].reshape(4, 2, 8, 128)
        cosines = twiddle_ref[0, parity * 32 : parity * 32 + 32, :].reshape(4, 1, 8, 128)
        sines = twiddle_ref[1, parity * 32 : parity * 32 + 32, :].reshape(4, 1, 8, 128)
        turned = jnp.concatenate(
            [(re * cosines + im * sines).reshape(64, 128), (im * cosines - re * sines).reshape(64, 128)], axis=1
        )
        halves.append(wide_dot(turned, plane_ref[parity, 0], plane_ref[parity, 1]))
    even_slot = (lax.broadcasted_iota(jnp.int32, (64, 128), 1) // 32) % 2 == 0
    for tile in range(2):
        a = halves[0][:, tile * 128 : (tile + 1) * 128]
        b = halves[1][:, tile * 128 : (tile + 1) * 128]
        put(2 * tile, jnp.where(even_slot, a, b))
        put(2 * tile + 1, jnp.where(even_slot, b, a))


def line_transform(held, flip, line_ref, staging, chunk):
    turned = []
    for g in range(2):
        block = jnp.concatenate([held[chunk, pl.ds(4 * g + f4, 32, stride=8), :] for f4 in range(4)], axis=0)
        across = block.T
        turned.append(jnp.concatenate([across[:64], across[64:]], axis=1))
    result = wide_dot(jnp.concatenate(turned, axis=0), line_ref[0], line_ref[1])
    lane = lax.broadcasted_iota(jnp.int32, (8, 128), 1)
    low_half, even_slot = lane < 64, (lane // 32) % 2 == 0
    for g in range(2):
        for k in range(2):
            for part in range(2):
                v = [
                    result[((g * 2 + k) * 4 + j) * 8 : ((g * 2 + k) * 4 + j + 1) * 8, part * 128 : (part + 1) * 128]
                    for j in range(4)
                ]
                w = [None] * 4
                for j in range(2):
                    w[j] = jnp.where(low_half, v[j], pltpu.roll(v[j + 2], 64, 1))
                    w[j + 2] = jnp.where(low_half, pltpu.roll(v[j], 64, 1), v[j + 2])
                for j in (0, 2):
                    first = jnp.where(even_slot, w[j], pltpu.roll(w[j + 1], 32, 1))
                    second = jnp.where(even_slot, pltpu.roll(w[j], 96, 1), w[j + 1])
                    start = pl.multiple_of(16 * lax.rem(k + flip, 2), 16) + part
                    staging[8 * chunk + 4 * g + j, pl.ds(start, 8, stride=2), :] = first
                    staging[8 * chunk + 4 * g + j + 1, pl.ds(start, 8, stride=2), :] = second


def whole_kernel(
    one_ref, two_ref, fold_hbm, twiddle_hbm, plane_hbm, line_hbm, out_ref,
    staged, sites, spins, fields, outgoing, held, staging, fold_ref, twiddle_ref, plane_ref, line_ref,
    load_sems, send_sems, recv_sems, last_send, last_recv, own_sem,
):
    ta, me = lax.axis_index("ta"), lax.axis_index("xyz")
    barrier = pltpu.get_barrier_semaphore()

    def to_peers(action):
        def one(step, carry):
            turn, near = 1 - step // 8, lax.rem(step, 8)
            offset = 4 + (1 - 2 * lax.rem(near, 2)) * ((near + 1) // 2)
            action(8 * lax.rem(me // 8 + turn, 2) + lax.rem(me + offset, 8))
            return carry

        lax.fori_loop(0, 15, one, 0)

    to_peers(lambda q: pl.semaphore_signal(barrier, inc=1, device_id={"xyz": q}, device_id_type=MESH))

    copies = []
    for chunk in range(8):
        rows = 36 * PITCH
        source = (one_ref, two_ref)[chunk // 4]
        copies.append(
            pltpu.make_async_copy(
                source.at[pl.ds((chunk % 4) * rows, rows)], staged.at[pl.ds(chunk * rows, rows)], load_sems.at[chunk]
            )
        )
        copies[-1].start()
    tables = [
        pltpu.make_async_copy(source, target, load_sems.at[8 + index])
        for index, (source, target) in enumerate(
            ((fold_hbm, fold_ref), (twiddle_hbm.at[0:2], twiddle_ref), (plane_hbm, plane_ref), (line_hbm, line_ref))
        )
    ]
    for table in tables:
        table.start()

    def greet(offset, carry):
        pl.semaphore_signal(
            barrier, inc=1, device_id={"ta": lax.rem(ta + offset, 16)}, device_id_type=MESH
        )
        return carry

    lax.fori_loop(1, 16, greet, 0)

    def crossing(chunk, source, target, peer):
        return pltpu.make_async_remote_copy(
            src_ref=outgoing.at[chunk, target],
            dst_ref=held.at[chunk, pl.ds(pl.multiple_of(source * 16, 16), 16)],
            send_sem=send_sems.at[chunk, target],
            recv_sem=recv_sems.at[chunk, source],
            device_id={"xyz": peer},
            device_id_type=MESH,
        )

    for chunk in range(8):
        copies[chunk].wait()
        widen(chunk, staged, sites)
    for chunk in range(2):
        contract_half(chunk, sites, spins, fields)
        if chunk == 0:
            for table in tables:
                table.wait()

        def put(kh, rows, chunk=chunk):
            outgoing[chunk, 4 * kh : 4 * kh + 4] = rows.reshape(4, 16, 128)

        plane_transform(chunk, fields, fold_ref, twiddle_ref, plane_ref, put)
        if chunk == 0:
            pl.semaphore_wait(barrier, 30)

        to_peers(lambda q, chunk=chunk: crossing(chunk, me, q, q).start())
        held[chunk, pl.ds(pl.multiple_of(me * 16, 16), 16), :] = outgoing[chunk, me]
    flip = lax.rem(me // 4, 2)

    def leaving(f, f16, source):
        return pltpu.make_async_remote_copy(
            src_ref=staging.at[f16],
            dst_ref=out_ref.at[source],
            send_sem=last_send.at[f16],
            recv_sem=last_recv.at[source],
            device_id={"ta": f},
            device_id_type=MESH,
        )

    for chunk in range(2):

        def arrive(offset, carry, chunk=chunk):
            q = lax.rem(me + offset, 16)
            crossing(chunk, q, me, q).wait_recv()
            return carry

        lax.fori_loop(1, 16, arrive, 0)
        line_transform(held, flip, line_ref, staging, chunk)
        for f8 in range(8):
            f = 4 * (f8 // 2) + 2 * chunk + f8 % 2

            @pl.when(f != ta)
            def _(f=f, f16=8 * chunk + f8):
                leaving(f, f16, ta).start()

            @pl.when(f == ta)
            def _(f16=8 * chunk + f8):
                pltpu.make_async_copy(staging.at[f16], out_ref.at[ta], own_sem.at[0]).start()

    for chunk in range(2):

        def sent(offset, carry, chunk=chunk):
            q = lax.rem(me + offset, 16)
            crossing(chunk, me, q, q).wait_send()
            return carry

        lax.fori_loop(1, 16, sent, 0)
        for f8 in range(8):
            f = 4 * (f8 // 2) + 2 * chunk + f8 % 2

            @pl.when(f != ta)
            def _(f=f, f16=8 * chunk + f8):
                leaving(f, f16, ta).wait_send()

    pltpu.make_async_copy(staging.at[0], out_ref.at[ta], own_sem.at[0]).wait()

    def final(offset, carry):
        t = lax.rem(ta + offset, 16)
        leaving(t, 0, t).wait_recv()
        return carry

    lax.fori_loop(1, 16, final, 0)


def site_rows(prop):
    entries = prop.transpose(0, 2, 3, 1, 4).reshape(ENTRIES, 2, 16, 128)
    return entries.transpose(0, 2, 1, 3).reshape(ENTRIES * PITCH, 128)


def on_device(prop_one, prop_two):
    anywhere = pl.BlockSpec(memory_space=pl.ANY)
    rows = pl.pallas_call(
        whole_kernel,
        name="whole",
        out_shape=jax.ShapeDtypeStruct((16, 32, 128), jnp.float32),
        in_specs=[anywhere] * 6,
        out_specs=anywhere,
        scratch_shapes=[
            pltpu.VMEM((2 * ENTRIES * PITCH, 128), jnp.bfloat16),
            pltpu.VMEM((2 * ENTRIES * PITCH, 128), jnp.float32),
            pltpu.VMEM((8, 8, 8, 128), jnp.float32),
            pltpu.VMEM((256, 128), jnp.float32),
            pltpu.VMEM((2, 16, 16, 128), jnp.float32),
            pltpu.VMEM((2, 256, 128), jnp.float32),
            pltpu.VMEM((16, 32, 128), jnp.float32),
            pltpu.VMEM((2, 512, 256), jnp.bfloat16),
            pltpu.VMEM((2, 64, 128), jnp.float32),
            pltpu.VMEM((2, 2, 256, 256), jnp.bfloat16),
            pltpu.VMEM((2, 256, 256), jnp.bfloat16),
            pltpu.SemaphoreType.DMA((12,)),
            pltpu.SemaphoreType.DMA((2, 16)),
            pltpu.SemaphoreType.DMA((2, 16)),
            pltpu.SemaphoreType.DMA((16,)),
            pltpu.SemaphoreType.DMA((16,)),
            pltpu.SemaphoreType.DMA((1,)),
        ],
        compiler_params=pltpu.CompilerParams(
            collective_id=0, has_side_effects=True, vmem_limit_bytes=67_043_328 - (10650 << 10), flags=FLAGS
        ),
    )(
        site_rows(prop_one),
        site_rows(prop_two),
        jnp.asarray(fold_tables()),
        jnp.asarray(twiddle_tables()),
        jnp.asarray(plane_tables()),
        jnp.asarray(line_tables()),
    )
    return rows.reshape(16, 16, 2, 128).transpose(0, 2, 1, 3).reshape(16, 1, 2, 2048)


def solution(mesh):
    placed = (P("ta", None, None, None, "xyz"), P("ta", None, None, None, "xyz"))
    return jax.shard_map(
        on_device, mesh=mesh, in_specs=placed, out_specs=P(None, "ta", None, "xyz"), check_vma=False
    )
```

```python
import functools

import jax
import jax.numpy as jnp
import numpy as np
from jax import lax
from jax.experimental import pallas as pl
from jax.experimental.pallas import tpu as pltpu
from jax.sharding import PartitionSpec as P

L = 32
MESH = pl.DeviceIdType.MESH
ENTRIES = 144
FLAGS = {}
PITCH = 32

REVERSED = [3, 2, 1, 0]
SWAPPED = [2, 3, 0, 1]
LEFT_PHASE = [1j, -1.0, 1j, 1.0]
RIGHT_PHASE = [-1j, 1.0, -1j, -1.0]


def split_table(values):
    high = jnp.asarray(values, jnp.float32).astype(jnp.bfloat16)
    high_np = np.asarray(values, np.float32).astype(jnp.bfloat16).astype(np.float64)
    low = np.asarray(values - high_np, np.float32).astype(jnp.bfloat16)
    high = np.asarray(values, np.float32).astype(jnp.bfloat16)
    return high, low


def real_form(z):
    return np.stack([np.stack([z.real, -z.imag]), np.stack([z.imag, z.real])])


def fold_tables():
    result = []
    for chunk in range(2):
        table = np.zeros((2, 2, 4, 2, 8, 2, 8, 2, 8))
        for f8 in range(8):
            mu, nu = f8 // 2, 2 * chunk + f8 % 2
            phase = LEFT_PHASE[mu] * RIGHT_PHASE[nu]
            for parity in range(2):
                for m in range(4):
                    z = phase * np.exp(-2j * np.pi * np.arange(8) * (2 * m + parity) / 8)
                    form = real_form(z)
                    for x in range(2):
                        table[parity, :, m, x, f8, x, f8] = form
        result.append(np.concatenate(split_table(table.reshape(256, 256)), axis=0))
    return np.stack(result)


def twiddle_tables():
    kl = (2 * np.arange(4)[None, :] + np.arange(2)[:, None]).reshape(8)
    angle = 2 * np.pi * kl[:, None] * np.repeat(np.arange(4), 32)[None, :] / 32
    rows = np.stack([np.cos(angle), np.sin(angle)])
    rows = np.repeat(rows[:, :, None, :], 8, axis=2).reshape(2, 64, 128).astype(np.float32)
    return np.concatenate([rows] * 8)


def plane_tables():
    yl, z = np.arange(4)[:, None], np.arange(32)[None, :]
    kz = np.array([4 * high + low for low in range(4) for high in range(8)])
    result = []
    for parity in range(2):
        table = np.zeros((2, 128, 2, 4, 32))
        for tile in range(2):
            for slot in range(4):
                part, kh = slot // 2, 2 * tile + (slot % 2 if parity == 0 else 1 - slot % 2)
                w = np.exp(-2j * np.pi * ((yl * kh / 4)[:, :, None] + z[:, :, None] * kz[None, None, :] / 32)) / 32
                form = real_form(w.reshape(128, 32))
                table[:, :, tile, slot] = form[part]
        result.append(np.stack(split_table(table.reshape(256, 256))))
    return np.stack(result)


def line_tables():
    w = np.exp(-2j * np.pi * np.arange(32)[:, None] * np.arange(32)[None, :] / 32) / np.sqrt(32)
    form = real_form(w)
    table = np.zeros((2, 4, 32, 2, 4, 32))
    for f4 in range(4):
        table[:, f4, :, :, f4] = form.transpose(1, 2, 0, 3)
    return np.stack(split_table(table.reshape(256, 256)))


def split_values(values):
    high = values.astype(jnp.bfloat16)
    low = (values - high.astype(jnp.float32)).astype(jnp.bfloat16)
    return high, low


def dot(a, b):
    return jnp.dot(a, b, preferred_element_type=jnp.float32)


def wide_dot(values, high_table, low_table):
    rows = values.shape[0]
    high, low = split_values(values)
    both = dot(jnp.concatenate([high, low], axis=0), high_table)
    return both[:rows] + both[rows:] + dot(high, low_table)


def widen(chunk, staged, sites):
    rows = 36 * PITCH
    base = chunk * rows

    def one(index, carry):
        start = pl.multiple_of(base + index * 384, 128)
        sites[pl.ds(start, 384), :] = staged[pl.ds(start, 384), :].astype(jnp.float32)
        return carry

    lax.fori_loop(0, rows // 384, one, 0)


def combine(reversed_pair, p):
    if reversed_pair:
        even, odd = p[0] + p[2], p[1] + p[3]
        return even + odd, even - odd
    outer, inner = p[0] - p[3], p[1] - p[2]
    return outer - inner, outer + inner


def contract_half(half, sites, spins, fields):
    def one_spin(index, carry):
        h, t = index // 4, lax.rem(index, 4)
        paired = 3 - t if half == 0 else lax.rem(t + 2, 4)
        first_base = pl.multiple_of(16 * h + 3 * PITCH * t, 16)
        second_base = pl.multiple_of(16 * h + 3 * PITCH * paired, 16)

        def entry(prop, part, row, k):
            start = (prop * ENTRIES + row * 12 + k) * PITCH + part
            return sites[pl.ds((first_base, second_base)[prop] + start, 8, stride=2), :]

        sums = [[None] * 4 for _ in range(2)]
        for i in range(3):
            for k in range(3):
                first = [[entry(0, part, 3 * s + i, k) for part in range(2)] for s in range(4)]
                second = [[entry(1, part, 3 * s + i, k) for part in range(2)] for s in range(4)]
                for s in range(4):
                    for side, pair in enumerate((REVERSED, SWAPPED)):
                        ar, ai = first[pair[s]]
                        br, bi = second[s]
                        re = ar * br + ai * bi
                        im = ai * br - ar * bi
                        old = sums[side][s]
                        sums[side][s] = [re, im] if old is None else [old[0] + re, old[1] + im]
        for side in range(2):
            for part in range(2):
                pair = combine(side == 0, [sums[side][s][part] for s in range(4)])
                for other in range(2):
                    spins[index, 4 * side + 2 * other + part] = pair[other]
        return carry

    lax.fori_loop(0, 8, one_spin, 0, unroll=2)
    for h in range(2):
        for side in range(2):
            for left in range(2):
                for part in range(2):
                    pair = combine(half == 0, [spins[4 * h + t, 4 * side + 2 * left + part] for t in range(4)])
                    for other in range(2):
                        row = h * 128 + ((2 * (2 * side + left) + other) * 2 + part) * 8
                        fields[row : row + 8, :] = pair[other]


def plane_transform(chunk, fields, fold_ref, twiddle_ref, plane_ref, put):
    high, low = split_values(fields[...])
    folded = dot(fold_ref[chunk], jnp.concatenate([high, low], axis=1))
    folded = folded[:256, :128] + folded[:256, 128:] + folded[256:, :128]
    halves = []
    for parity in range(2):
        re = folded[parity * 128 : parity * 128 + 64].reshape(4, 2, 8, 128)
        im = folded[parity * 128 + 64 : parity * 128 + 128].reshape(4, 2, 8, 128)
        cosines = twiddle_ref[0, parity * 32 : parity * 32 + 32, :].reshape(4, 1, 8, 128)
        sines = twiddle_ref[1, parity * 32 : parity * 32 + 32, :].reshape(4, 1, 8, 128)
        turned = jnp.concatenate(
            [(re * cosines + im * sines).reshape(64, 128), (im * cosines - re * sines).reshape(64, 128)], axis=1
        )
        halves.append(wide_dot(turned, plane_ref[parity, 0], plane_ref[parity, 1]))
    even_slot = (lax.broadcasted_iota(jnp.int32, (64, 128), 1) // 32) % 2 == 0
    for tile in range(2):
        a = halves[0][:, tile * 128 : (tile + 1) * 128]
        b = halves[1][:, tile * 128 : (tile + 1) * 128]
        put(2 * tile, jnp.where(even_slot, a, b))
        put(2 * tile + 1, jnp.where(even_slot, b, a))


def line_transform(held, flip, line_ref, staging, chunk):
    turned = []
    for g in range(2):
        block = jnp.concatenate([held[chunk, pl.ds(4 * g + f4, 32, stride=8), :] for f4 in range(4)], axis=0)
        across = block.T
        turned.append(jnp.concatenate([across[:64], across[64:]], axis=1))
    result = wide_dot(jnp.concatenate(turned, axis=0), line_ref[0], line_ref[1])
    lane = lax.broadcasted_iota(jnp.int32, (8, 128), 1)
    low_half, even_slot = lane < 64, (lane // 32) % 2 == 0
    for g in range(2):
        for k in range(2):
            for part in range(2):
                v = [
                    result[((g * 2 + k) * 4 + j) * 8 : ((g * 2 + k) * 4 + j + 1) * 8, part * 128 : (part + 1) * 128]
                    for j in range(4)
                ]
                w = [None] * 4
                for j in range(2):
                    w[j] = jnp.where(low_half, v[j], pltpu.roll(v[j + 2], 64, 1))
                    w[j + 2] = jnp.where(low_half, pltpu.roll(v[j], 64, 1), v[j + 2])
                for j in (0, 2):
                    first = jnp.where(even_slot, w[j], pltpu.roll(w[j + 1], 32, 1))
                    second = jnp.where(even_slot, pltpu.roll(w[j], 96, 1), w[j + 1])
                    start = pl.multiple_of(16 * lax.rem(k + flip, 2), 16) + part
                    staging[8 * chunk + 4 * g + j, pl.ds(start, 8, stride=2), :] = first
                    staging[8 * chunk + 4 * g + j + 1, pl.ds(start, 8, stride=2), :] = second


def whole_kernel(
    one_ref, two_ref, fold_hbm, twiddle_hbm, plane_hbm, line_hbm, out_ref,
    staged, sites, spins, fields, outgoing, held, staging, fold_ref, twiddle_ref, plane_ref, line_ref,
    load_sems, send_sems, recv_sems, last_send, last_recv, own_sem,
):
    ta, me = lax.axis_index("ta"), lax.axis_index("xyz")
    barrier = pltpu.get_barrier_semaphore()

    z = lax.rem(me, 8)
    own_x = me - z
    rows_of_x = (8 - own_x, own_x)

    def to_peers(action):
        for low in (0, 4):
            for row in rows_of_x:
                for other in range(low, low + 4):
                    if row is rows_of_x[0]:
                        action(row + other)
                        continue

                    @pl.when(other != z)
                    def _(q=row + other):
                        action(q)

    to_peers(lambda q: pl.semaphore_signal(barrier, inc=1, device_id={"xyz": q}, device_id_type=MESH))

    copies = []
    for chunk in range(8):
        rows = 36 * PITCH
        source = (one_ref, two_ref)[chunk // 4]
        copies.append(
            pltpu.make_async_copy(
                source.at[pl.ds((chunk % 4) * rows, rows)], staged.at[pl.ds(chunk * rows, rows)], load_sems.at[chunk]
            )
        )
        copies[-1].start()
    tables = [
        pltpu.make_async_copy(source, target, load_sems.at[8 + index])
        for index, (source, target) in enumerate(
            ((fold_hbm, fold_ref), (twiddle_hbm.at[0:2], twiddle_ref), (plane_hbm, plane_ref), (line_hbm, line_ref))
        )
    ]
    for table in tables:
        table.start()

    for offset in range(1, 16):
        pl.semaphore_signal(
            barrier, inc=1, device_id={"ta": lax.rem(ta + offset, 16)}, device_id_type=MESH
        )

    def crossing(chunk, source, target, peer):
        return pltpu.make_async_remote_copy(
            src_ref=outgoing.at[chunk, target],
            dst_ref=held.at[chunk, pl.ds(pl.multiple_of(source * 16, 16), 16)],
            send_sem=send_sems.at[chunk, target],
            recv_sem=recv_sems.at[chunk, source],
            device_id={"xyz": peer},
            device_id_type=MESH,
        )

    for chunk in range(8):
        copies[chunk].wait()
        widen(chunk, staged, sites)
    for chunk in range(2):
        contract_half(chunk, sites, spins, fields)
        if chunk == 0:
            for table in tables:
                table.wait()

        def put(kh, rows, chunk=chunk):
            outgoing[chunk, 4 * kh : 4 * kh + 4] = rows.reshape(4, 16, 128)

        plane_transform(chunk, fields, fold_ref, twiddle_ref, plane_ref, put)
        if chunk == 0:
            pl.semaphore_wait(barrier, 30)

        to_peers(lambda q, chunk=chunk: crossing(chunk, me, q, q).start())
        held[chunk, pl.ds(pl.multiple_of(me * 16, 16), 16), :] = outgoing[chunk, me]
    flip = lax.rem(me // 4, 2)

    def leaving(f, f16, source):
        return pltpu.make_async_remote_copy(
            src_ref=staging.at[f16],
            dst_ref=out_ref.at[source],
            send_sem=last_send.at[f16],
            recv_sem=last_recv.at[source],
            device_id={"ta": f},
            device_id_type=MESH,
        )

    for chunk in range(2):

        def arrive(offset, carry, chunk=chunk):
            q = lax.rem(me + offset, 16)
            crossing(chunk, q, me, q).wait_recv()
            return carry

        lax.fori_loop(1, 16, arrive, 0)
        line_transform(held, flip, line_ref, staging, chunk)
        for f8 in range(8):
            f = 4 * (f8 // 2) + 2 * chunk + f8 % 2

            @pl.when(f != ta)
            def _(f=f, f16=8 * chunk + f8):
                leaving(f, f16, ta).start()

            @pl.when(f == ta)
            def _(f16=8 * chunk + f8):
                pltpu.make_async_copy(staging.at[f16], out_ref.at[ta], own_sem.at[0]).start()

    for chunk in range(2):

        def sent(offset, carry, chunk=chunk):
            q = lax.rem(me + offset, 16)
            crossing(chunk, me, q, q).wait_send()
            return carry

        lax.fori_loop(1, 16, sent, 0)
        for f8 in range(8):
            f = 4 * (f8 // 2) + 2 * chunk + f8 % 2

            @pl.when(f != ta)
            def _(f=f, f16=8 * chunk + f8):
                leaving(f, f16, ta).wait_send()

    pltpu.make_async_copy(staging.at[0], out_ref.at[ta], own_sem.at[0]).wait()

    def final(offset, carry):
        t = lax.rem(ta + offset, 16)
        leaving(t, 0, t).wait_recv()
        return carry

    lax.fori_loop(1, 16, final, 0)


def site_rows(prop):
    entries = prop.transpose(0, 2, 3, 1, 4).reshape(ENTRIES, 2, 16, 128)
    return entries.transpose(0, 2, 1, 3).reshape(ENTRIES * PITCH, 128)


def on_device(prop_one, prop_two):
    anywhere = pl.BlockSpec(memory_space=pl.ANY)
    rows = pl.pallas_call(
        whole_kernel,
        name="whole",
        out_shape=jax.ShapeDtypeStruct((16, 32, 128), jnp.float32),
        in_specs=[anywhere] * 6,
        out_specs=anywhere,
        scratch_shapes=[
            pltpu.VMEM((2 * ENTRIES * PITCH, 128), jnp.bfloat16),
            pltpu.VMEM((2 * ENTRIES * PITCH, 128), jnp.float32),
            pltpu.VMEM((8, 8, 8, 128), jnp.float32),
            pltpu.VMEM((256, 128), jnp.float32),
            pltpu.VMEM((2, 16, 16, 128), jnp.float32),
            pltpu.VMEM((2, 256, 128), jnp.float32),
            pltpu.VMEM((16, 32, 128), jnp.float32),
            pltpu.VMEM((2, 512, 256), jnp.bfloat16),
            pltpu.VMEM((2, 64, 128), jnp.float32),
            pltpu.VMEM((2, 2, 256, 256), jnp.bfloat16),
            pltpu.VMEM((2, 256, 256), jnp.bfloat16),
            pltpu.SemaphoreType.DMA((12,)),
            pltpu.SemaphoreType.DMA((2, 16)),
            pltpu.SemaphoreType.DMA((2, 16)),
            pltpu.SemaphoreType.DMA((16,)),
            pltpu.SemaphoreType.DMA((16,)),
            pltpu.SemaphoreType.DMA((1,)),
        ],
        compiler_params=pltpu.CompilerParams(
            collective_id=0, has_side_effects=True, vmem_limit_bytes=67_043_328 - (10650 << 10), flags=FLAGS
        ),
    )(
        site_rows(prop_one),
        site_rows(prop_two),
        jnp.asarray(fold_tables()),
        jnp.asarray(twiddle_tables()),
        jnp.asarray(plane_tables()),
        jnp.asarray(line_tables()),
    )
    return rows.reshape(16, 16, 2, 128).transpose(0, 2, 1, 3).reshape(16, 1, 2, 2048)


def solution(mesh):
    placed = (P("ta", None, None, None, "xyz"), P("ta", None, None, None, "xyz"))
    return jax.shard_map(
        on_device, mesh=mesh, in_specs=placed, out_specs=P(None, "ta", None, "xyz"), check_vma=False
    )
```

```python
import functools

import jax
import jax.numpy as jnp
import numpy as np
from jax import lax
from jax.experimental import pallas as pl
from jax.experimental.pallas import tpu as pltpu
from jax.sharding import PartitionSpec as P

L = 32
MESH = pl.DeviceIdType.MESH
ENTRIES = 144
FLAGS = {}
PITCH = 32

REVERSED = [3, 2, 1, 0]
SWAPPED = [2, 3, 0, 1]
LEFT_PHASE = [1j, -1.0, 1j, 1.0]
RIGHT_PHASE = [-1j, 1.0, -1j, -1.0]


def split_table(values):
    high = jnp.asarray(values, jnp.float32).astype(jnp.bfloat16)
    high_np = np.asarray(values, np.float32).astype(jnp.bfloat16).astype(np.float64)
    low = np.asarray(values - high_np, np.float32).astype(jnp.bfloat16)
    high = np.asarray(values, np.float32).astype(jnp.bfloat16)
    return high, low


def real_form(z):
    return np.stack([np.stack([z.real, -z.imag]), np.stack([z.imag, z.real])])


def fold_tables():
    result = []
    for chunk in range(2):
        table = np.zeros((2, 2, 4, 2, 8, 2, 8, 2, 8))
        for f8 in range(8):
            mu, nu = f8 // 2, 2 * chunk + f8 % 2
            phase = LEFT_PHASE[mu] * RIGHT_PHASE[nu]
            for parity in range(2):
                for m in range(4):
                    z = phase * np.exp(-2j * np.pi * np.arange(8) * (2 * m + parity) / 8)
                    form = real_form(z)
                    for x in range(2):
                        table[parity, :, m, x, f8, x, f8] = form
        result.append(np.concatenate(split_table(table.reshape(256, 256)), axis=0))
    return np.stack(result)


def twiddle_tables():
    kl = (2 * np.arange(4)[None, :] + np.arange(2)[:, None]).reshape(8)
    angle = 2 * np.pi * kl[:, None] * np.repeat(np.arange(4), 32)[None, :] / 32
    rows = np.stack([np.cos(angle), np.sin(angle)])
    rows = np.repeat(rows[:, :, None, :], 8, axis=2).reshape(2, 64, 128).astype(np.float32)
    return np.concatenate([rows] * 8)


def plane_tables():
    yl, z = np.arange(4)[:, None], np.arange(32)[None, :]
    kz = np.array([4 * high + low for low in range(4) for high in range(8)])
    result = []
    for parity in range(2):
        table = np.zeros((2, 128, 2, 4, 32))
        for tile in range(2):
            for slot in range(4):
                part, kh = slot // 2, 2 * tile + (slot % 2 if parity == 0 else 1 - slot % 2)
                w = np.exp(-2j * np.pi * ((yl * kh / 4)[:, :, None] + z[:, :, None] * kz[None, None, :] / 32)) / 32
                form = real_form(w.reshape(128, 32))
                table[:, :, tile, slot] = form[part]
        result.append(np.stack(split_table(table.reshape(256, 256))))
    return np.stack(result)


def line_tables():
    w = np.exp(-2j * np.pi * np.arange(32)[:, None] * np.arange(32)[None, :] / 32) / np.sqrt(32)
    form = real_form(w)
    table = np.zeros((2, 4, 32, 2, 4, 32))
    for f4 in range(4):
        table[:, f4, :, :, f4] = form.transpose(1, 2, 0, 3)
    return np.stack(split_table(table.reshape(256, 256)))


def split_values(values):
    high = values.astype(jnp.bfloat16)
    low = (values - high.astype(jnp.float32)).astype(jnp.bfloat16)
    return high, low


def dot(a, b):
    return jnp.dot(a, b, preferred_element_type=jnp.float32)


def wide_dot(values, high_table, low_table):
    rows = values.shape[0]
    high, low = split_values(values)
    both = dot(jnp.concatenate([high, low], axis=0), high_table)
    return both[:rows] + both[rows:] + dot(high, low_table)


def widen(chunk, staged, sites):
    rows = 36 * PITCH
    base = chunk * rows

    def one(index, carry):
        start = pl.multiple_of(base + index * 384, 128)
        sites[pl.ds(start, 384), :] = staged[pl.ds(start, 384), :].astype(jnp.float32)
        return carry

    lax.fori_loop(0, rows // 384, one, 0)


def combine(reversed_pair, p):
    if reversed_pair:
        even, odd = p[0] + p[2], p[1] + p[3]
        return even + odd, even - odd
    outer, inner = p[0] - p[3], p[1] - p[2]
    return outer - inner, outer + inner


def contract_half(half, sites, spins, fields):
    def one_spin(index, carry):
        h, t = index // 4, lax.rem(index, 4)
        paired = 3 - t if half == 0 else lax.rem(t + 2, 4)
        first_base = pl.multiple_of(16 * h + 3 * PITCH * t, 16)
        second_base = pl.multiple_of(16 * h + 3 * PITCH * paired, 16)

        def entry(prop, part, row, k):
            start = (prop * ENTRIES + row * 12 + k) * PITCH + part
            return sites[pl.ds((first_base, second_base)[prop] + start, 8, stride=2), :]

        sums = [[None] * 4 for _ in range(2)]
        for i in range(3):
            for k in range(3):
                first = [[entry(0, part, 3 * s + i, k) for part in range(2)] for s in range(4)]
                second = [[entry(1, part, 3 * s + i, k) for part in range(2)] for s in range(4)]
                for s in range(4):
                    for side, pair in enumerate((REVERSED, SWAPPED)):
                        ar, ai = first[pair[s]]
                        br, bi = second[s]
                        re = ar * br + ai * bi
                        im = ai * br - ar * bi
                        old = sums[side][s]
                        sums[side][s] = [re, im] if old is None else [old[0] + re, old[1] + im]
        for side in range(2):
            for part in range(2):
                pair = combine(side == 0, [sums[side][s][part] for s in range(4)])
                for other in range(2):
                    spins[index, 4 * side + 2 * other + part] = pair[other]
        return carry

    lax.fori_loop(0, 8, one_spin, 0, unroll=2)
    for h in range(2):
        for side in range(2):
            for left in range(2):
                for part in range(2):
                    pair = combine(half == 0, [spins[4 * h + t, 4 * side + 2 * left + part] for t in range(4)])
                    for other in range(2):
                        row = h * 128 + ((2 * (2 * side + left) + other) * 2 + part) * 8
                        fields[row : row + 8, :] = pair[other]


def plane_transform(chunk, fields, fold_ref, twiddle_ref, plane_ref, put):
    high, low = split_values(fields[...])
    folded = dot(fold_ref[chunk], jnp.concatenate([high, low], axis=1))
    folded = folded[:256, :128] + folded[:256, 128:] + folded[256:, :128]
    halves = []
    for parity in range(2):
        re = folded[parity * 128 : parity * 128 + 64].reshape(4, 2, 8, 128)
        im = folded[parity * 128 + 64 : parity * 128 + 128].reshape(4, 2, 8, 128)
        cosines = twiddle_ref[0, parity * 32 : parity * 32 + 32, :].reshape(4, 1, 8, 128)
        sines = twiddle_ref[1, parity * 32 : parity * 32 + 32, :].reshape(4, 1, 8, 128)
        turned = jnp.concatenate(
            [(re * cosines + im * sines).reshape(64, 128), (im * cosines - re * sines).reshape(64, 128)], axis=1
        )
        halves.append(wide_dot(turned, plane_ref[parity, 0], plane_ref[parity, 1]))
    even_slot = (lax.broadcasted_iota(jnp.int32, (64, 128), 1) // 32) % 2 == 0
    for tile in range(2):
        a = halves[0][:, tile * 128 : (tile + 1) * 128]
        b = halves[1][:, tile * 128 : (tile + 1) * 128]
        put(2 * tile, jnp.where(even_slot, a, b))
        put(2 * tile + 1, jnp.where(even_slot, b, a))


def line_transform(held, flip, line_ref, staging, chunk, g):
    block = jnp.concatenate([held[chunk, pl.ds(4 * g + f4, 32, stride=8), :] for f4 in range(4)], axis=0)
    across = block.T
    result = wide_dot(jnp.concatenate([across[:64], across[64:]], axis=1), line_ref[0], line_ref[1])
    lane = lax.broadcasted_iota(jnp.int32, (8, 128), 1)
    low_half, even_slot = lane < 64, (lane // 32) % 2 == 0
    for k in range(2):
        for part in range(2):
            v = [
                result[(k * 4 + j) * 8 : (k * 4 + j + 1) * 8, part * 128 : (part + 1) * 128]
                for j in range(4)
            ]
            w = [None] * 4
            for j in range(2):
                w[j] = jnp.where(low_half, v[j], pltpu.roll(v[j + 2], 64, 1))
                w[j + 2] = jnp.where(low_half, pltpu.roll(v[j], 64, 1), v[j + 2])
            for j in (0, 2):
                first = jnp.where(even_slot, w[j], pltpu.roll(w[j + 1], 32, 1))
                second = jnp.where(even_slot, pltpu.roll(w[j], 96, 1), w[j + 1])
                start = pl.multiple_of(16 * lax.rem(k + flip, 2), 16) + part
                staging[8 * chunk + 4 * g + j, pl.ds(start, 8, stride=2), :] = first
                staging[8 * chunk + 4 * g + j + 1, pl.ds(start, 8, stride=2), :] = second


def whole_kernel(
    one_ref, two_ref, fold_hbm, twiddle_hbm, plane_hbm, line_hbm, out_ref,
    staged, sites, spins, fields, outgoing, held, staging, fold_ref, twiddle_ref, plane_ref, line_ref,
    load_sems, send_sems, recv_sems, last_send, last_recv, own_sem,
):
    ta, me = lax.axis_index("ta"), lax.axis_index("xyz")
    barrier = pltpu.get_barrier_semaphore()

    z = lax.rem(me, 8)
    own_x = me - z
    rows_of_x = (8 - own_x, own_x)

    def to_peers(action):
        for low in (0, 4):
            for row in rows_of_x:
                for other in range(low, low + 4):
                    if row is rows_of_x[0]:
                        action(row + other)
                        continue

                    @pl.when(other != z)
                    def _(q=row + other):
                        action(q)

    to_peers(lambda q: pl.semaphore_signal(barrier, inc=1, device_id={"xyz": q}, device_id_type=MESH))

    copies = []
    for chunk in range(8):
        rows = 36 * PITCH
        source = (one_ref, two_ref)[chunk // 4]
        copies.append(
            pltpu.make_async_copy(
                source.at[pl.ds((chunk % 4) * rows, rows)], staged.at[pl.ds(chunk * rows, rows)], load_sems.at[chunk]
            )
        )
        copies[-1].start()
    tables = [
        pltpu.make_async_copy(source, target, load_sems.at[8 + index])
        for index, (source, target) in enumerate(
            ((fold_hbm, fold_ref), (twiddle_hbm.at[0:2], twiddle_ref), (plane_hbm, plane_ref), (line_hbm, line_ref))
        )
    ]
    for table in tables:
        table.start()

    for offset in range(1, 16):
        pl.semaphore_signal(
            barrier, inc=1, device_id={"ta": lax.rem(ta + offset, 16)}, device_id_type=MESH
        )

    def crossing(chunk, source, target, peer):
        return pltpu.make_async_remote_copy(
            src_ref=outgoing.at[chunk, target],
            dst_ref=held.at[chunk, pl.ds(pl.multiple_of(source * 16, 16), 16)],
            send_sem=send_sems.at[chunk, target],
            recv_sem=recv_sems.at[chunk, source],
            device_id={"xyz": peer},
            device_id_type=MESH,
        )

    for chunk in range(8):
        copies[chunk].wait()
        widen(chunk, staged, sites)
    for chunk in range(2):
        contract_half(chunk, sites, spins, fields)
        if chunk == 0:
            for table in tables:
                table.wait()

        def put(kh, rows, chunk=chunk):
            outgoing[chunk, 4 * kh : 4 * kh + 4] = rows.reshape(4, 16, 128)

        plane_transform(chunk, fields, fold_ref, twiddle_ref, plane_ref, put)
        if chunk == 0:
            pl.semaphore_wait(barrier, 30)

        to_peers(lambda q, chunk=chunk: crossing(chunk, me, q, q).start())
        held[chunk, pl.ds(pl.multiple_of(me * 16, 16), 16), :] = outgoing[chunk, me]
    flip = lax.rem(me // 4, 2)

    def leaving(f, f16, source):
        return pltpu.make_async_remote_copy(
            src_ref=staging.at[f16],
            dst_ref=out_ref.at[source],
            send_sem=last_send.at[f16],
            recv_sem=last_recv.at[source],
            device_id={"ta": f},
            device_id_type=MESH,
        )

    for chunk in range(2):

        def arrive(offset, carry, chunk=chunk):
            q = lax.rem(me + offset, 16)
            crossing(chunk, q, me, q).wait_recv()
            return carry

        lax.fori_loop(1, 16, arrive, 0)
        for f8 in range(8):
            if f8 % 4 == 0:
                line_transform(held, flip, line_ref, staging, chunk, f8 // 4)
            f = 4 * (f8 // 2) + 2 * chunk + f8 % 2

            @pl.when(f != ta)
            def _(f=f, f16=8 * chunk + f8):
                leaving(f, f16, ta).start()

            @pl.when(f == ta)
            def _(f16=8 * chunk + f8):
                pltpu.make_async_copy(staging.at[f16], out_ref.at[ta], own_sem.at[0]).start()

    for chunk in range(2):

        def sent(offset, carry, chunk=chunk):
            q = lax.rem(me + offset, 16)
            crossing(chunk, me, q, q).wait_send()
            return carry

        lax.fori_loop(1, 16, sent, 0)
        for f8 in range(8):
            f = 4 * (f8 // 2) + 2 * chunk + f8 % 2

            @pl.when(f != ta)
            def _(f=f, f16=8 * chunk + f8):
                leaving(f, f16, ta).wait_send()

    pltpu.make_async_copy(staging.at[0], out_ref.at[ta], own_sem.at[0]).wait()

    def final(offset, carry):
        t = lax.rem(ta + offset, 16)
        leaving(t, 0, t).wait_recv()
        return carry

    lax.fori_loop(1, 16, final, 0)


def site_rows(prop):
    entries = prop.transpose(0, 2, 3, 1, 4).reshape(ENTRIES, 2, 16, 128)
    return entries.transpose(0, 2, 1, 3).reshape(ENTRIES * PITCH, 128)


def on_device(prop_one, prop_two):
    anywhere = pl.BlockSpec(memory_space=pl.ANY)
    rows = pl.pallas_call(
        whole_kernel,
        name="whole",
        out_shape=jax.ShapeDtypeStruct((16, 32, 128), jnp.float32),
        in_specs=[anywhere] * 6,
        out_specs=anywhere,
        scratch_shapes=[
            pltpu.VMEM((2 * ENTRIES * PITCH, 128), jnp.bfloat16),
            pltpu.VMEM((2 * ENTRIES * PITCH, 128), jnp.float32),
            pltpu.VMEM((8, 8, 8, 128), jnp.float32),
            pltpu.VMEM((256, 128), jnp.float32),
            pltpu.VMEM((2, 16, 16, 128), jnp.float32),
            pltpu.VMEM((2, 256, 128), jnp.float32),
            pltpu.VMEM((16, 32, 128), jnp.float32),
            pltpu.VMEM((2, 512, 256), jnp.bfloat16),
            pltpu.VMEM((2, 64, 128), jnp.float32),
            pltpu.VMEM((2, 2, 256, 256), jnp.bfloat16),
            pltpu.VMEM((2, 256, 256), jnp.bfloat16),
            pltpu.SemaphoreType.DMA((12,)),
            pltpu.SemaphoreType.DMA((2, 16)),
            pltpu.SemaphoreType.DMA((2, 16)),
            pltpu.SemaphoreType.DMA((16,)),
            pltpu.SemaphoreType.DMA((16,)),
            pltpu.SemaphoreType.DMA((1,)),
        ],
        compiler_params=pltpu.CompilerParams(
            collective_id=0, has_side_effects=True, vmem_limit_bytes=67_043_328 - (10650 << 10), flags=FLAGS
        ),
    )(
        site_rows(prop_one),
        site_rows(prop_two),
        jnp.asarray(fold_tables()),
        jnp.asarray(twiddle_tables()),
        jnp.asarray(plane_tables()),
        jnp.asarray(line_tables()),
    )
    return rows.reshape(16, 16, 2, 128).transpose(0, 2, 1, 3).reshape(16, 1, 2, 2048)


def solution(mesh):
    placed = (P("ta", None, None, None, "xyz"), P("ta", None, None, None, "xyz"))
    return jax.shard_map(
        on_device, mesh=mesh, in_specs=placed, out_specs=P(None, "ta", None, "xyz"), check_vma=False
    )
```

```python
import functools

import jax
import jax.numpy as jnp
import numpy as np
from jax import lax
from jax.experimental import pallas as pl
from jax.experimental.pallas import tpu as pltpu
from jax.sharding import PartitionSpec as P

L = 32
MESH = pl.DeviceIdType.MESH
ENTRIES = 144
FLAGS = {}
PITCH = 32

REVERSED = [3, 2, 1, 0]
SWAPPED = [2, 3, 0, 1]
LEFT_PHASE = [1j, -1.0, 1j, 1.0]
RIGHT_PHASE = [-1j, 1.0, -1j, -1.0]


def split_table(values):
    high = jnp.asarray(values, jnp.float32).astype(jnp.bfloat16)
    high_np = np.asarray(values, np.float32).astype(jnp.bfloat16).astype(np.float64)
    low = np.asarray(values - high_np, np.float32).astype(jnp.bfloat16)
    high = np.asarray(values, np.float32).astype(jnp.bfloat16)
    return high, low


def real_form(z):
    return np.stack([np.stack([z.real, -z.imag]), np.stack([z.imag, z.real])])


def fold_tables():
    result = []
    for chunk in range(2):
        table = np.zeros((2, 2, 4, 2, 8, 2, 8, 2, 8))
        for f8 in range(8):
            mu, nu = f8 // 2, 2 * chunk + f8 % 2
            phase = LEFT_PHASE[mu] * RIGHT_PHASE[nu]
            for parity in range(2):
                for m in range(4):
                    z = phase * np.exp(-2j * np.pi * np.arange(8) * (2 * m + parity) / 8)
                    form = real_form(z)
                    for x in range(2):
                        table[parity, :, m, x, f8, x, f8] = form
        result.append(np.concatenate(split_table(table.reshape(256, 256)), axis=0))
    return np.stack(result)


def twiddle_tables():
    kl = (2 * np.arange(4)[None, :] + np.arange(2)[:, None]).reshape(8)
    angle = 2 * np.pi * kl[:, None] * np.repeat(np.arange(4), 32)[None, :] / 32
    rows = np.stack([np.cos(angle), np.sin(angle)])
    rows = np.repeat(rows[:, :, None, :], 8, axis=2).reshape(2, 64, 128).astype(np.float32)
    return np.concatenate([rows] * 8)


def plane_tables():
    yl, z = np.arange(4)[:, None], np.arange(32)[None, :]
    kz = np.array([4 * high + low for low in range(4) for high in range(8)])
    result = []
    for parity in range(2):
        table = np.zeros((2, 128, 2, 4, 32))
        for tile in range(2):
            for slot in range(4):
                part, kh = slot // 2, 2 * tile + (slot % 2 if parity == 0 else 1 - slot % 2)
                w = np.exp(-2j * np.pi * ((yl * kh / 4)[:, :, None] + z[:, :, None] * kz[None, None, :] / 32)) / 32
                form = real_form(w.reshape(128, 32))
                table[:, :, tile, slot] = form[part]
        result.append(np.stack(split_table(table.reshape(256, 256))))
    return np.stack(result)


def line_tables():
    w = np.exp(-2j * np.pi * np.arange(32)[:, None] * np.arange(32)[None, :] / 32) / np.sqrt(32)
    form = real_form(w)
    table = np.zeros((2, 4, 32, 2, 4, 32))
    for f4 in range(4):
        table[:, f4, :, :, f4] = form.transpose(1, 2, 0, 3)
    return np.stack(split_table(table.reshape(256, 256)))


def split_values(values):
    high = values.astype(jnp.bfloat16)
    low = (values - high.astype(jnp.float32)).astype(jnp.bfloat16)
    return high, low


def dot(a, b):
    return jnp.dot(a, b, preferred_element_type=jnp.float32)


def wide_dot(values, high_table, low_table):
    rows = values.shape[0]
    high, low = split_values(values)
    both = dot(jnp.concatenate([high, low], axis=0), high_table)
    return both[:rows] + both[rows:] + dot(high, low_table)


def widen(chunk, staged, sites):
    rows = 36 * PITCH
    base = chunk * rows

    def one(index, carry):
        start = pl.multiple_of(base + index * 384, 128)
        sites[pl.ds(start, 384), :] = staged[pl.ds(start, 384), :].astype(jnp.float32)
        return carry

    lax.fori_loop(0, rows // 384, one, 0)


def combine(reversed_pair, p):
    if reversed_pair:
        even, odd = p[0] + p[2], p[1] + p[3]
        return even + odd, even - odd
    outer, inner = p[0] - p[3], p[1] - p[2]
    return outer - inner, outer + inner


def contract_half(half, sites, spins, fields):
    def one_spin(index, carry):
        h, t = index // 4, lax.rem(index, 4)
        paired = 3 - t if half == 0 else lax.rem(t + 2, 4)
        first_base = pl.multiple_of(16 * h + 3 * PITCH * t, 16)
        second_base = pl.multiple_of(16 * h + 3 * PITCH * paired, 16)

        def entry(prop, part, row, k):
            start = (prop * ENTRIES + row * 12 + k) * PITCH + part
            return sites[pl.ds((first_base, second_base)[prop] + start, 8, stride=2), :]

        sums = [[None] * 4 for _ in range(2)]
        for i in range(3):
            for k in range(3):
                first = [[entry(0, part, 3 * s + i, k) for part in range(2)] for s in range(4)]
                second = [[entry(1, part, 3 * s + i, k) for part in range(2)] for s in range(4)]
                for s in range(4):
                    for side, pair in enumerate((REVERSED, SWAPPED)):
                        ar, ai = first[pair[s]]
                        br, bi = second[s]
                        re = ar * br + ai * bi
                        im = ai * br - ar * bi
                        old = sums[side][s]
                        sums[side][s] = [re, im] if old is None else [old[0] + re, old[1] + im]
        for side in range(2):
            for part in range(2):
                pair = combine(side == 0, [sums[side][s][part] for s in range(4)])
                for other in range(2):
                    spins[index, 4 * side + 2 * other + part] = pair[other]
        return carry

    lax.fori_loop(0, 8, one_spin, 0, unroll=2)
    for h in range(2):
        for side in range(2):
            for left in range(2):
                for part in range(2):
                    pair = combine(half == 0, [spins[4 * h + t, 4 * side + 2 * left + part] for t in range(4)])
                    for other in range(2):
                        row = h * 128 + ((2 * (2 * side + left) + other) * 2 + part) * 8
                        fields[row : row + 8, :] = pair[other]


def plane_transform(chunk, fields, fold_ref, twiddle_ref, plane_ref, put):
    high, low = split_values(fields[...])
    folded = dot(fold_ref[chunk], jnp.concatenate([high, low], axis=1))
    folded = folded[:256, :128] + folded[:256, 128:] + folded[256:, :128]
    halves = []
    for parity in range(2):
        re = folded[parity * 128 : parity * 128 + 64].reshape(4, 2, 8, 128)
        im = folded[parity * 128 + 64 : parity * 128 + 128].reshape(4, 2, 8, 128)
        cosines = twiddle_ref[0, parity * 32 : parity * 32 + 32, :].reshape(4, 1, 8, 128)
        sines = twiddle_ref[1, parity * 32 : parity * 32 + 32, :].reshape(4, 1, 8, 128)
        turned = jnp.concatenate(
            [(re * cosines + im * sines).reshape(64, 128), (im * cosines - re * sines).reshape(64, 128)], axis=1
        )
        halves.append(wide_dot(turned, plane_ref[parity, 0], plane_ref[parity, 1]))
    even_slot = (lax.broadcasted_iota(jnp.int32, (64, 128), 1) // 32) % 2 == 0
    for tile in range(2):
        a = halves[0][:, tile * 128 : (tile + 1) * 128]
        b = halves[1][:, tile * 128 : (tile + 1) * 128]
        put(2 * tile, jnp.where(even_slot, a, b))
        put(2 * tile + 1, jnp.where(even_slot, b, a))


def line_transform(held, flip, line_ref, staging, chunk):
    turned = []
    for g in range(2):
        block = jnp.concatenate([held[chunk, pl.ds(4 * g + f4, 32, stride=8), :] for f4 in range(4)], axis=0)
        across = block.T
        turned.append(jnp.concatenate([across[:64], across[64:]], axis=1))
    result = wide_dot(jnp.concatenate(turned, axis=0), line_ref[0], line_ref[1])
    lane = lax.broadcasted_iota(jnp.int32, (8, 128), 1)
    low_half, even_slot = lane < 64, (lane // 32) % 2 == 0
    for g in range(2):
        for k in range(2):
            for part in range(2):
                v = [
                    result[((g * 2 + k) * 4 + j) * 8 : ((g * 2 + k) * 4 + j + 1) * 8, part * 128 : (part + 1) * 128]
                    for j in range(4)
                ]
                w = [None] * 4
                for j in range(2):
                    w[j] = jnp.where(low_half, v[j], pltpu.roll(v[j + 2], 64, 1))
                    w[j + 2] = jnp.where(low_half, pltpu.roll(v[j], 64, 1), v[j + 2])
                for j in (0, 2):
                    first = jnp.where(even_slot, w[j], pltpu.roll(w[j + 1], 32, 1))
                    second = jnp.where(even_slot, pltpu.roll(w[j], 96, 1), w[j + 1])
                    start = pl.multiple_of(16 * lax.rem(k + flip, 2), 16) + part
                    staging[8 * chunk + 4 * g + j, pl.ds(start, 8, stride=2), :] = first
                    staging[8 * chunk + 4 * g + j + 1, pl.ds(start, 8, stride=2), :] = second


def whole_kernel(
    one_ref, two_ref, fold_hbm, twiddle_hbm, plane_hbm, line_hbm, out_ref,
    staged, sites, spins, fields, outgoing, held, staging, fold_ref, twiddle_ref, plane_ref, line_ref,
    load_sems, send_sems, recv_sems, last_send, last_recv, own_sem,
):
    ta, me = lax.axis_index("ta"), lax.axis_index("xyz")
    barrier = pltpu.get_barrier_semaphore()

    z = lax.rem(me, 8)
    own_x = me - z
    rows_of_x = (8 - own_x, own_x)

    def to_peers(action):
        for low in (0, 4):
            for row in rows_of_x:
                for other in range(low, low + 4):
                    if row is rows_of_x[0]:
                        action(row + other)
                        continue

                    @pl.when(other != z)
                    def _(q=row + other):
                        action(q)

    to_peers(lambda q: pl.semaphore_signal(barrier, inc=1, device_id={"xyz": q}, device_id_type=MESH))

    copies = []
    for chunk in range(8):
        rows = 36 * PITCH
        source = (one_ref, two_ref)[chunk // 4]
        copies.append(
            pltpu.make_async_copy(
                source.at[pl.ds((chunk % 4) * rows, rows)], staged.at[pl.ds(chunk * rows, rows)], load_sems.at[chunk]
            )
        )
        copies[-1].start()
    tables = [
        pltpu.make_async_copy(source, target, load_sems.at[8 + index])
        for index, (source, target) in enumerate(
            ((fold_hbm, fold_ref), (twiddle_hbm.at[0:2], twiddle_ref), (plane_hbm, plane_ref), (line_hbm, line_ref))
        )
    ]
    for table in tables:
        table.start()

    for offset in range(1, 16):
        pl.semaphore_signal(
            barrier, inc=1, device_id={"ta": lax.rem(ta + offset, 16)}, device_id_type=MESH
        )

    def crossing(chunk, source, target, peer):
        return pltpu.make_async_remote_copy(
            src_ref=outgoing.at[chunk, target],
            dst_ref=held.at[chunk, pl.ds(pl.multiple_of(source * 16, 16), 16)],
            send_sem=send_sems.at[chunk, target],
            recv_sem=recv_sems.at[chunk, source],
            device_id={"xyz": peer},
            device_id_type=MESH,
        )

    for chunk in range(8):
        copies[chunk].wait()
        widen(chunk, staged, sites)
    for chunk in range(2):
        contract_half(chunk, sites, spins, fields)
        if chunk == 0:
            for table in tables:
                table.wait()

        def put(kh, rows, chunk=chunk):
            outgoing[chunk, 4 * kh : 4 * kh + 4] = rows.reshape(4, 16, 128)

        plane_transform(chunk, fields, fold_ref, twiddle_ref, plane_ref, put)
        first_here = z // 4 == 1 - chunk

        @pl.when(first_here)
        def _():
            pl.semaphore_wait(barrier, 30)
            to_peers(lambda q: crossing(0, me, q, q).start())

        if chunk == 1:
            to_peers(lambda q: crossing(1, me, q, q).start())
        held[chunk, pl.ds(pl.multiple_of(me * 16, 16), 16), :] = outgoing[chunk, me]
    flip = lax.rem(me // 4, 2)

    def leaving(f, f16, source):
        return pltpu.make_async_remote_copy(
            src_ref=staging.at[f16],
            dst_ref=out_ref.at[source],
            send_sem=last_send.at[f16],
            recv_sem=last_recv.at[source],
            device_id={"ta": f},
            device_id_type=MESH,
        )

    for chunk in range(2):

        def arrive(offset, carry, chunk=chunk):
            q = lax.rem(me + offset, 16)
            crossing(chunk, q, me, q).wait_recv()
            return carry

        lax.fori_loop(1, 16, arrive, 0)
        line_transform(held, flip, line_ref, staging, chunk)
        for f8 in range(8):
            f = 4 * (f8 // 2) + 2 * chunk + f8 % 2

            @pl.when(f != ta)
            def _(f=f, f16=8 * chunk + f8):
                leaving(f, f16, ta).start()

            @pl.when(f == ta)
            def _(f16=8 * chunk + f8):
                pltpu.make_async_copy(staging.at[f16], out_ref.at[ta], own_sem.at[0]).start()

    for chunk in range(2):

        def sent(offset, carry, chunk=chunk):
            q = lax.rem(me + offset, 16)
            crossing(chunk, me, q, q).wait_send()
            return carry

        lax.fori_loop(1, 16, sent, 0)
        for f8 in range(8):
            f = 4 * (f8 // 2) + 2 * chunk + f8 % 2

            @pl.when(f != ta)
            def _(f=f, f16=8 * chunk + f8):
                leaving(f, f16, ta).wait_send()

    pltpu.make_async_copy(staging.at[0], out_ref.at[ta], own_sem.at[0]).wait()

    def final(offset, carry):
        t = lax.rem(ta + offset, 16)
        leaving(t, 0, t).wait_recv()
        return carry

    lax.fori_loop(1, 16, final, 0)


def site_rows(prop):
    entries = prop.transpose(0, 2, 3, 1, 4).reshape(ENTRIES, 2, 16, 128)
    return entries.transpose(0, 2, 1, 3).reshape(ENTRIES * PITCH, 128)


def on_device(prop_one, prop_two):
    anywhere = pl.BlockSpec(memory_space=pl.ANY)
    rows = pl.pallas_call(
        whole_kernel,
        name="whole",
        out_shape=jax.ShapeDtypeStruct((16, 32, 128), jnp.float32),
        in_specs=[anywhere] * 6,
        out_specs=anywhere,
        scratch_shapes=[
            pltpu.VMEM((2 * ENTRIES * PITCH, 128), jnp.bfloat16),
            pltpu.VMEM((2 * ENTRIES * PITCH, 128), jnp.float32),
            pltpu.VMEM((8, 8, 8, 128), jnp.float32),
            pltpu.VMEM((256, 128), jnp.float32),
            pltpu.VMEM((2, 16, 16, 128), jnp.float32),
            pltpu.VMEM((2, 256, 128), jnp.float32),
            pltpu.VMEM((16, 32, 128), jnp.float32),
            pltpu.VMEM((2, 512, 256), jnp.bfloat16),
            pltpu.VMEM((2, 64, 128), jnp.float32),
            pltpu.VMEM((2, 2, 256, 256), jnp.bfloat16),
            pltpu.VMEM((2, 256, 256), jnp.bfloat16),
            pltpu.SemaphoreType.DMA((12,)),
            pltpu.SemaphoreType.DMA((2, 16)),
            pltpu.SemaphoreType.DMA((2, 16)),
            pltpu.SemaphoreType.DMA((16,)),
            pltpu.SemaphoreType.DMA((16,)),
            pltpu.SemaphoreType.DMA((1,)),
        ],
        compiler_params=pltpu.CompilerParams(
            collective_id=0, has_side_effects=True, vmem_limit_bytes=67_043_328 - (10650 << 10), flags=FLAGS
        ),
    )(
        site_rows(prop_one),
        site_rows(prop_two),
        jnp.asarray(fold_tables()),
        jnp.asarray(twiddle_tables()),
        jnp.asarray(plane_tables()),
        jnp.asarray(line_tables()),
    )
    return rows.reshape(16, 16, 2, 128).transpose(0, 2, 1, 3).reshape(16, 1, 2, 2048)


def solution(mesh):
    placed = (P("ta", None, None, None, "xyz"), P("ta", None, None, None, "xyz"))
    return jax.shard_map(
        on_device, mesh=mesh, in_specs=placed, out_specs=P(None, "ta", None, "xyz"), check_vma=False
    )
```
